512 devices in a mesh: cfg: 2 (over y), gx: 128 (over x, z), gy: 2 (over core).
Axes of the slice: x: 8, y: 2, z: 16, core: 2. Of those that a mesh axis runs over, the one named last changes fastest.
The devices are a block of a 8x8x16 slice.
Arguments:
- gauge_links: float32 [4, 12, 256, 16, 1024], P(None, None, ('cfg', 'gx'), 'gy'), parts along dimension 2, may hold values from -1 to 1, as said below
- momentum: float32 [8, 256, 16, 1024], P(None, ('cfg', 'gx'), 'gy'), parts along dimension 1, may hold values from -6 to 6
Outputs:
- new_momentum: float32 [8, 256, 16, 1024], P(None, ('cfg', 'gx'), 'gy'), parts along dimension 1
- new_link: float32 [12, 256, 16, 1024], P(None, ('cfg', 'gx'), 'gy'), parts along dimension 1
The draws below stay inside these ranges and needn't reach their ends.
There are 2 independent parts, one for each index of `cfg`. The reference program is written for one: setup_inputs(seed, part) draws one part's arguments, and reference() takes and returns one part's arrays. A program takes and returns all parts, laid end to end along the dimension named above; each array names one. Nothing has to cross between parts.
Inputs may be any that keep to these rules, and one draw needn't show every extreme that they name: `gauge_links`: for every direction and site the two rows are orthonormal complex 3-vectors up to rounding.
All inputs are finite; a program needn't handle non-finite values.
Results may differ from the reference program's by a relative error of at most 0.0003.
Values sent between devices are 32-bit elements; how exact they have to be, the bound alone decides.
A program may use at most 128 MiB of HBM per device.

```python
import math
import jax
import jax.numpy as jnp
from jax import lax

NZ = 32
NT = 32
NX = 128
NY = 16
ZT = 1024


def draw_gauge_links(key, part):
    shape_site = (4, NX, NY, NZ * NT)
    angles = jax.random.uniform(jax.random.fold_in(key, 21), (8,) + shape_site, jnp.float32)
    angles = 2.0 * math.pi * angles
    angle_a = angles[0]
    angle_b = angles[1]
    angle_c = angles[2]
    phase_one = angles[3]
    phase_two = angles[4]
    phase_three = angles[5]
    phase_q = angles[6]
    phase_r = angles[7]
    first_mag = jnp.stack([jnp.cos(angle_a), jnp.sin(angle_a) * jnp.cos(angle_b), jnp.sin(angle_a) * jnp.sin(angle_b)])
    other_mag = jnp.stack([-jnp.sin(angle_a), jnp.cos(angle_a) * jnp.cos(angle_b), jnp.cos(angle_a) * jnp.sin(angle_b)])
    third_mag = jnp.stack([jnp.zeros_like(angle_b), -jnp.sin(angle_b), jnp.cos(angle_b)])
    phases = jnp.stack([phase_one, phase_two, phase_three])
    first_re = first_mag * jnp.cos(phases)
    first_im = first_mag * jnp.sin(phases)
    other_re = other_mag * jnp.cos(phases + phase_q[None])
    other_im = other_mag * jnp.sin(phases + phase_q[None])
    third_re = third_mag * jnp.cos(phases + phase_r[None])
    third_im = third_mag * jnp.sin(phases + phase_r[None])
    weight_one = jnp.cos(angle_c)[None]
    weight_two = jnp.sin(angle_c)[None]
    second_re = weight_one * other_re + weight_two * third_re
    second_im = weight_one * other_im + weight_two * third_im
    rows_re = jnp.stack([first_re, second_re], axis=1)
    rows_im = jnp.stack([first_im, second_im], axis=1)
    rows_re = jnp.moveaxis(rows_re, 0, 2)
    rows_im = jnp.moveaxis(rows_im, 0, 2)
    return jnp.concatenate([rows_re.reshape((4, 6, NX, NY, NZ * NT)), rows_im.reshape((4, 6, NX, NY, NZ * NT))], axis=1)


def level_of(own_key, extent, pieces, low, largest):
    def one(position, shards_of):
        draws = jax.random.uniform(jax.random.fold_in(jax.random.fold_in(own_key, 6), position), (shards_of,), jnp.float32, low / len(pieces), largest / len(pieces))
        return jnp.repeat(jnp.exp(draws), extent[position] // shards_of).reshape((-1,) + (1,) * (len(extent) - position - 1))

    gain = one(*pieces[0])
    for cut in pieces[1:]:
        gain = gain * one(*cut)
    return gain


def scatter_about(stream_key, shape, spread, most, shards=(), kind=jnp.bfloat16):
    array = spread * jax.random.normal(stream_key, shape, jnp.float32)
    if shards:
        array = array * level_of(stream_key, shape, shards, -0.22, 0.18)
    return jnp.clip(array, -most, most).astype(kind)


def setup_inputs(seed: int = 0, part: int = 0) -> dict:
    seeds = jax.random.split(jax.random.key(seed), 3)
    part_splits = jax.random.split(jax.random.fold_in(seeds[2], part), 3)
    gauge_links = draw_gauge_links(jax.random.fold_in(jax.random.fold_in(seeds[2], part), 71), part)
    momentum = scatter_about(part_splits[1], (8, NX, NY, ZT), 1.0, 6.0, ((1, 128), (2, 2)), jnp.float32)
    return dict(gauge_links=gauge_links, momentum=momentum)


coupling = 6.0
step_force = 0.3
step_link = 0.15
kernel_mass = 0.01

def entry_prod(left_mat, right_mat):
    return lax.optimization_barrier(jnp.sum(left_mat[:, :, None] * right_mat[None, :, :], axis=1))

def su3_product(left_pair, right_pair):
    return (entry_prod(left_pair[0], right_pair[0]) - entry_prod(left_pair[1], right_pair[1]), entry_prod(left_pair[0], right_pair[1]) + entry_prod(left_pair[1], right_pair[0]))

def adjoint(matrix):
    return (jnp.swapaxes(matrix[0], 0, 1), -jnp.swapaxes(matrix[1], 0, 1))

def unpack(packed):
    rest = packed.shape[1:]
    rows_re = packed[0:6].reshape((2, 3) + rest)
    rows_im = packed[6:12].reshape((2, 3) + rest)
    third_re = []
    third_im = []
    for column in range(3):
        first_col = (column + 1) % 3
        second_col = (column + 2) % 3
        cross_re = rows_re[0, first_col] * rows_re[1, second_col] - rows_im[0, first_col] * rows_im[1, second_col] - (rows_re[0, second_col] * rows_re[1, first_col] - rows_im[0, second_col] * rows_im[1, first_col])
        cross_im = rows_re[0, first_col] * rows_im[1, second_col] + rows_im[0, first_col] * rows_re[1, second_col] - (rows_re[0, second_col] * rows_im[1, first_col] + rows_im[0, second_col] * rows_re[1, first_col])
        third_re.append(cross_re)
        third_im.append(-cross_im)
    return (jnp.concatenate([rows_re, jnp.stack(third_re)[None]], axis=0), jnp.concatenate([rows_im, jnp.stack(third_im)[None]], axis=0))

def algebra_parts(matrix):
    whole_re, whole_im = matrix
    root_three = math.sqrt(3.0)
    parts_list = [whole_im[1, 0] + whole_im[0, 1], whole_re[0, 1] - whole_re[1, 0], whole_im[0, 0] - whole_im[1, 1], whole_im[2, 0] + whole_im[0, 2], whole_re[0, 2] - whole_re[2, 0], whole_im[2, 1] + whole_im[1, 2], whole_re[1, 2] - whole_re[2, 1], (whole_im[0, 0] + whole_im[1, 1] - 2.0 * whole_im[2, 2]) / root_three]
    return jnp.stack(parts_list)

def algebra_matrix(parts):
    root_inv = 1.0 / math.sqrt(3.0)
    zero_part = jnp.zeros_like(parts[0])
    herm_re = jnp.stack([jnp.stack([0.5 * (parts[2] + root_inv * parts[7]), 0.5 * parts[0], 0.5 * parts[3]]), jnp.stack([0.5 * parts[0], 0.5 * (root_inv * parts[7] - parts[2]), 0.5 * parts[5]]), jnp.stack([0.5 * parts[3], 0.5 * parts[5], -root_inv * parts[7]])])
    herm_im = jnp.stack([jnp.stack([zero_part, -0.5 * parts[1], -0.5 * parts[4]]), jnp.stack([0.5 * parts[1], zero_part, -0.5 * parts[6]]), jnp.stack([0.5 * parts[4], 0.5 * parts[6], zero_part])])
    return (herm_re, herm_im)

def link_exp(parts):
    herm_re, herm_im = algebra_matrix(parts)
    gen_re = -0.25 * step_link * herm_im
    gen_im = 0.25 * step_link * herm_re
    eye_mat = jnp.eye(3, dtype=jnp.float32)[:, :, None, None, None] + jnp.zeros_like(gen_re)
    series = (eye_mat, jnp.zeros_like(gen_re))
    for series_order in range(6, 0, -1):
        grown = su3_product((gen_re, gen_im), series)
        series = (eye_mat + grown[0] / series_order, grown[1] / series_order)
    for square_step in range(2):
        series = su3_product(series, series)
    return series

def move_field(field_data, lattice_dim, offset):
    if lattice_dim < 2:
        return jnp.roll(field_data, -offset, axis=2 + lattice_dim)
    leading = field_data.shape[:-1]
    lattice = field_data.reshape(leading + (NZ, NT))
    lattice = jnp.roll(lattice, -offset, axis=len(leading) + lattice_dim - 2)
    return lattice.reshape(field_data.shape)

def moved(matrix, lattice_dim, offset):
    return (move_field(matrix[0], lattice_dim, offset), move_field(matrix[1], lattice_dim, offset))

def sine_squares(length):
    phase_angle = jnp.arange(length, dtype=jnp.int32).astype(jnp.float32) * (math.pi / length)
    return jnp.sin(phase_angle) * jnp.sin(phase_angle)

def reference(gauge_links, momentum):
    link_x = unpack(gauge_links[0])
    staple_re = jnp.zeros_like(link_x[0])
    staple_im = jnp.zeros_like(link_x[0])
    for direction in range(1, 4):
        link_nu = unpack(gauge_links[direction])
        ahead_nu = moved(link_nu, 0, 1)
        upper_staple = su3_product(su3_product(ahead_nu, adjoint(moved(link_x, direction, 1))), adjoint(link_nu))
        lower_staple = su3_product(su3_product(adjoint(moved(ahead_nu, direction, -1)), adjoint(moved(link_x, direction, -1))), moved(link_nu, direction, -1))
        staple_re = staple_re + upper_staple[0] + lower_staple[0]
        staple_im = staple_im + upper_staple[1] + lower_staple[1]
    loop_sum = su3_product(link_x, (staple_re, staple_im))
    force_parts = coupling / 6.0 * algebra_parts(loop_sum)
    new_momentum = momentum - step_force * force_parts
    lattice = new_momentum.reshape((8, NX, NY, NZ, NT))
    spectrum = jnp.fft.fftn(lattice, axes=(1, 2, 3, 4))
    plane_part = sine_squares(NZ)[:, None] + sine_squares(NT)[None, :]
    denom = kernel_mass + 4.0 * (sine_squares(NX)[:, None, None, None] + sine_squares(NY)[None, :, None, None] + plane_part[None, None, :, :])
    kernel_values = 4.0 / denom
    smooth = jnp.real(jnp.fft.ifftn(spectrum * kernel_values[None], axes=(1, 2, 3, 4))).astype(jnp.float32)
    smooth = smooth.reshape(new_momentum.shape)
    rotation = link_exp(smooth)
    updated = su3_product(rotation, link_x)
    rest = new_momentum.shape[1:]
    new_link = jnp.concatenate([updated[0][0:2].reshape((6,) + rest), updated[1][0:2].reshape((6,) + rest)], axis=0)
    return (new_momentum, new_link)
```

```python
import functools
import math

import jax
import jax.numpy as jnp
import numpy as np
from jax import lax
from jax.experimental import pallas as pl
from jax.experimental.pallas import tpu as pltpu
from jax.sharding import PartitionSpec as P

NZ = 32
NT = 32
LANES = 128

coupling = 6.0
step_force = 0.3
step_link = 0.15
kernel_mass = 0.01

f32 = jnp.float32
bf16 = jnp.bfloat16
VMEM = pl.BlockSpec(memory_space=pltpu.VMEM)
PARAMS = dict(vmem_limit_bytes=60 * 1024 * 1024)


def hartley(length):
    index = np.arange(length)
    angle = 2.0 * np.pi * (np.outer(index, index) % length) / length
    return np.cos(angle) + np.sin(angle)


def in_two(table):
    high = jnp.asarray(table, f32).astype(bf16)
    return high, (jnp.asarray(table, f32) - high.astype(f32)).astype(bf16)


def cdot(lefts, rights, conj_left=False, conj_right=False):
    re = im = None
    for (a, b), (c, d) in zip(lefts, rights):
        same = conj_left == conj_right
        re_term = a * c - b * d if same else a * c + b * d
        if not conj_left and not conj_right:
            im_term = a * d + b * c
        elif conj_left and not conj_right:
            im_term = a * d - b * c
        elif conj_right and not conj_left:
            im_term = b * c - a * d
        else:
            im_term = -(a * d + b * c)
        re = re_term if re is None else re + re_term
        im = im_term if im is None else im + im_term
    return re, im


def product(left, right, adj_left=False, adj_right=False):
    out = []
    for r in range(3):
        row = []
        lefts = [left[k][r] for k in range(3)] if adj_left else [left[r][k] for k in range(3)]
        for c in range(3):
            rights = [right[c][k] for k in range(3)] if adj_right else [right[k][c] for k in range(3)]
            row.append(cdot(lefts, rights, adj_left, adj_right))
        out.append(row)
    return out


def with_third(rows):
    third = []
    for k in range(3):
        i, j = (k + 1) % 3, (k + 2) % 3
        (a, b), (c, d) = rows[0][i], rows[1][j]
        (e, f), (g, h) = rows[0][j], rows[1][i]
        third.append(((a * c - b * d) - (e * g - f * h), (e * h + f * g) - (a * d + b * c)))
    return [rows[0], rows[1], third]


def matrix_of(get):
    return with_third([[(get(3 * r + k), get(6 + 3 * r + k)) for k in range(3)] for r in range(2)])


def algebra_parts(m):
    inv_root = 1.0 / math.sqrt(3.0)
    return [
        m[1][0][1] + m[0][1][1],
        m[0][1][0] - m[1][0][0],
        m[0][0][1] - m[1][1][1],
        m[2][0][1] + m[0][2][1],
        m[0][2][0] - m[2][0][0],
        m[2][1][1] + m[1][2][1],
        m[1][2][0] - m[2][1][0],
        (m[0][0][1] + m[1][1][1] - 2.0 * m[2][2][1]) * inv_root,
    ]


def split_dot(value, high_ref, low_ref, columns):
    high = value.astype(bf16)
    low = (value - high.astype(f32)).astype(bf16)
    table = high_ref[:, columns]
    return (
        jnp.dot(high, table, preferred_element_type=f32)
        + jnp.dot(low, table, preferred_element_type=f32)
        + jnp.dot(high, low_ref[:, columns], preferred_element_type=f32)
    )


def table_kernel(within_ref, across_ref, high_ref, low_ref):
    def block(z, carry):
        full = within_ref[...] * across_ref[pl.ds(z, 1), :]
        high = full.astype(bf16)
        rows = pl.ds(pl.multiple_of(z * NT, NT), NT)
        high_ref[rows, :] = high
        low_ref[rows, :] = (full - high.astype(f32)).astype(bf16)
        return carry

    lax.fori_loop(0, NZ, block, 0)


def plane_tables():
    sites = NZ * NT
    within = np.tile(hartley(NT), (1, NZ)).astype(np.float32)
    across = np.repeat(hartley(NZ), NT, axis=1).astype(np.float32)
    return pl.pallas_call(
        table_kernel,
        out_shape=[jax.ShapeDtypeStruct((sites, sites), bf16)] * 2,
        in_specs=[VMEM] * 2,
        out_specs=[VMEM] * 2,
        cost_estimate=pl.CostEstimate(flops=4 * sites * sites, bytes_accessed=8 * sites * sites, transcendentals=0),
        compiler_params=pltpu.CompilerParams(**PARAMS),
        name="plane_tables",
    )(jnp.asarray(within), jnp.asarray(across))


def force_kernel(
    links_ref, ahead_ref, rows_ref, corner_ref, momentum_ref, high_ref, low_ref,
    new_ref, spectrum_ref, partial_ref, staple_ref, behind_ref, edge_ref,
):
    tiles = new_ref.shape[2] // LANES
    lane = lax.broadcasted_iota(jnp.int32, (8, LANES), 1)
    sublane = lax.broadcasted_iota(jnp.int32, (8, LANES), 0)
    t_site = lane % NT

    edge_x = matrix_of(lambda e: rows_ref[12 + e])
    edge_y = matrix_of(lambda e: rows_ref[24 + e])
    edge_ahead = matrix_of(lambda e: corner_ref[e])
    edge = product(product(edge_x, edge_ahead), edge_y, adj_left=True)
    for r in range(3):
        for k in range(3):
            edge_ref[3 * r + k] = edge[r][k][0]
            edge_ref[9 + 3 * r + k] = edge[r][k][1]

    def first(i, carry):
        here = pl.ds(pl.multiple_of(i * LANES, LANES), LANES)
        after = pl.ds(pl.multiple_of(lax.rem(i + 1, tiles) * LANES, LANES), LANES)
        link_x = matrix_of(lambda e: links_ref[0, e, :, here])

        def moved_y(e):
            top = jnp.broadcast_to(rows_ref[e, pl.ds(i, 1), :], (8, LANES))
            return jnp.where(sublane == 7, top, pltpu.roll(links_ref[0, e, :, here], 7, 0))

        def moved_z(e):
            return jnp.where(
                lane < LANES - NT,
                pltpu.roll(links_ref[0, e, :, here], LANES - NT, 1),
                pltpu.roll(links_ref[0, e, :, after], LANES - NT, 1),
            )

        def moved_t(e):
            value = links_ref[0, e, :, here]
            return jnp.where(
                t_site == NT - 1, pltpu.roll(value, NT - 1, 1), pltpu.roll(value, LANES - 1, 1)
            )

        totals = None
        sums = None
        for nu, moved in ((1, moved_y), (2, moved_z), (3, moved_t)):
            link_nu = matrix_of(lambda e: links_ref[nu, e, :, here])
            ahead = matrix_of(lambda e: ahead_ref[nu - 1, e, :, here])
            path = product(link_x, ahead)
            lower = product(path, link_nu, adj_left=True)
            upper = product(path, product(link_nu, matrix_of(moved)), adj_right=True)
            parts = algebra_parts(upper)
            totals = parts if totals is None else [a + b for a, b in zip(totals, parts)]
            flat = [lower[r][k][p] for p in range(2) for r in range(3) for k in range(3)]
            if nu == 2:
                for e in range(18):
                    behind_ref[e, :, here] = flat[e]
                continue
            if nu == 1:
                flat = [
                    jnp.where(
                        sublane == 0,
                        jnp.broadcast_to(edge_ref[e, pl.ds(i, 1), :], (8, LANES)),
                        pltpu.roll(flat[e], 1, 0),
                    )
                    for e in range(18)
                ]
            else:
                flat = [
                    jnp.where(t_site == 0, pltpu.roll(v, LANES - NT + 1, 1), pltpu.roll(v, 1, 1))
                    for v in flat
                ]
            sums = flat if sums is None else [a + b for a, b in zip(sums, flat)]
        for e in range(18):
            staple_ref[e, :, here] = sums[e]
        for a in range(8):
            partial_ref[a, :, here] = totals[a]
        return carry

    lax.fori_loop(0, tiles, first, 0)

    def second(i, carry):
        here = pl.ds(pl.multiple_of(i * LANES, LANES), LANES)
        before = pl.ds(pl.multiple_of(lax.rem(i + tiles - 1, tiles) * LANES, LANES), LANES)
        flat = [
            staple_ref[e, :, here]
            + jnp.where(
                lane >= NT,
                pltpu.roll(behind_ref[e, :, here], NT, 1),
                pltpu.roll(behind_ref[e, :, before], NT, 1),
            )
            for e in range(18)
        ]
        staple = [[(flat[3 * r + k], flat[9 + 3 * r + k]) for k in range(3)] for r in range(3)]
        link_x = matrix_of(lambda e: links_ref[0, e, :, here])
        parts = algebra_parts(product(link_x, staple))
        for a in range(8):
            force = (coupling / 6.0) * (partial_ref[a, :, here] + parts[a])
            new_ref[a, :, here] = momentum_ref[a, :, here] - step_force * force
        return carry

    lax.fori_loop(0, tiles, second, 0)

    count = new_ref.shape[0] * new_ref.shape[1]
    half = tiles // 2
    value = new_ref[...].reshape(count, tiles * LANES)
    for pair in range(tiles // 2):
        columns = slice(pair * 2 * LANES, (pair + 1) * 2 * LANES)
        out = split_dot(value, high_ref, low_ref, columns)
        for side in range(2):
            tile = 2 * pair + side
            spectrum_ref[tile // half, pl.ds(tile % half, count, stride=half), :] = out[
                :, side * LANES : (side + 1) * LANES
            ]


def finish_kernel(filtered_ref, links_ref, high_ref, low_ref, new_ref, smooth_ref):
    tiles = new_ref.shape[2] // LANES
    half = tiles // 2
    count = 64
    pieces = [
        filtered_ref[tile // half, pl.ds(tile % half, count, stride=half), :] for tile in range(tiles)
    ]
    value = jnp.concatenate(pieces, axis=1)
    for pair in range(tiles // 2):
        columns = slice(pair * 2 * LANES, (pair + 1) * 2 * LANES)
        smooth_ref[:, columns] = split_dot(value, high_ref, low_ref, columns)
    root_inv = 1.0 / math.sqrt(3.0)
    scale = 0.25 * step_link * 0.5

    def one(i, carry):
        here = pl.ds(pl.multiple_of(i * LANES, LANES), LANES)
        s = [smooth_ref[pl.ds(8 * a, 8), here] * scale for a in range(8)]
        eighth = root_inv * s[7]
        h00, h11, h22 = eighth + s[2], eighth - s[2], -2.0 * eighth
        a01, b01 = s[0], -s[1]
        a02, b02 = s[3], -s[4]
        a12, b12 = s[5], -s[6]
        n01 = a01 * a01 + b01 * b01
        n02 = a02 * a02 + b02 * b02
        n12 = a12 * a12 + b12 * b12
        p = 0.5 * (h00 * h00 + h11 * h11 + h22 * h22) + (n01 + n02 + n12)
        m_re = a01 * a12 - b01 * b12
        m_im = a01 * b12 + b01 * a12
        q = h00 * h11 * h22 + 2.0 * (m_re * a02 + m_im * b02) - h00 * n12 - h11 * n02 - h22 * n01
        pq = p * q
        pp = p * p
        c0 = (1.0 - q * q * (1.0 / 720.0), pq * (1.0 / 120.0) - q * (1.0 / 6.0))
        c1 = (q * (1.0 / 24.0) - pq * (1.0 / 360.0), 1.0 - p * (1.0 / 6.0) + pp * (1.0 / 120.0))
        c2 = (p * (1.0 / 24.0) - 0.5 - pp * (1.0 / 720.0), q * (1.0 / 120.0))

        def cm(u, v):
            return (u[0] * v[0] - u[1] * v[1], u[0] * v[1] + u[1] * v[0])

        for _ in range(2):
            s00, s11, s22 = cm(c0, c0), cm(c1, c1), cm(c2, c2)
            d01, d02, d12 = cm(c0, c1), cm(c0, c2), cm(c1, c2)
            c0, c1, c2 = (
                tuple(s00[x] + 2.0 * q * d12[x] for x in range(2)),
                tuple(2.0 * (d01[x] + p * d12[x]) + q * s22[x] for x in range(2)),
                tuple(2.0 * d02[x] + s11[x] + p * s22[x] for x in range(2)),
            )
        g00 = h00 * h00 + n01 + n02
        g11 = h11 * h11 + n01 + n12
        g01 = (a01 * (h00 + h11) + a02 * a12 + b02 * b12, b01 * (h00 + h11) + b02 * a12 - a02 * b12)
        g02 = (a02 * (h00 + h22) + m_re, b02 * (h00 + h22) + m_im)
        g12 = (a12 * (h11 + h22) + a01 * a02 + b01 * b02, b12 * (h11 + h22) + a01 * b02 - b01 * a02)

        def mix(h, g):
            first, second = cm(c1, h), cm(c2, g)
            return (first[0] + second[0], first[1] + second[1])

        def diagonal(h, g):
            return (c0[0] + c1[0] * h + c2[0] * g, c0[1] + c1[1] * h + c2[1] * g)

        rotation = [
            [diagonal(h00, g00), mix((a01, b01), g01), mix((a02, b02), g02)],
            [mix((a01, -b01), (g01[0], -g01[1])), diagonal(h11, g11), mix((a12, b12), g12)],
        ]
        link = matrix_of(lambda e: links_ref[e, :, here])
        for r in range(2):
            for k in range(3):
                re, im = cdot(rotation[r], [link[m][k] for m in range(3)])
                new_ref[3 * r + k, :, here] = re
                new_ref[6 + 3 * r + k, :, here] = im
        return carry

    lax.fori_loop(0, tiles, one, 0)


def filter_kernel(
    inner, outer, y_table,
    spectrum_ref, weight_ref, high_ref, low_ref, out_ref,
    both_ref, bands_ref, arrive_ref, whole_ref, done_ref, back_ref, rows_ref, halves_ref,
    pair_sems, inner_sems, outer_sems, outer_back_sems, inner_back_sems, pair_back_sems,
):
    me = lax.axis_index("gx")
    core = lax.axis_index("gy")
    other = 1 - core
    row = me // inner
    col = me % inner

    def at_col(d):
        return lax.rem(col + d, inner)

    def at_row(d):
        return lax.rem(row + d, outer)

    barrier = pltpu.get_barrier_semaphore()

    def greet_col(d, carry):
        pl.semaphore_signal(barrier, inc=1, device_id={"gx": row * inner + at_col(d)}, device_id_type=pl.DeviceIdType.MESH)
        return carry

    def greet_row(d, carry):
        pl.semaphore_signal(barrier, inc=1, device_id={"gx": at_row(d) * inner + col}, device_id_type=pl.DeviceIdType.MESH)
        return carry

    lax.fori_loop(1, inner, greet_col, 0)
    lax.fori_loop(1, outer, greet_row, 0)
    pl.semaphore_signal(barrier, inc=1, device_id={"gy": other}, device_id_type=pl.DeviceIdType.MESH)
    pl.semaphore_wait(barrier, inner + outer - 1)

    def exchange(count, sems, source, target, device, own):
        def copy(d):
            return pltpu.make_async_remote_copy(
                src_ref=source(d), dst_ref=target, send_sem=sems.at[0, d], recv_sem=sems.at[1, d],
                device_id=device(d), device_id_type=pl.DeviceIdType.MESH,
            )

        def begin(d, carry):
            copy(d).start()
            return carry

        def finish(d, carry):
            copy(d).wait()
            return carry

        lax.fori_loop(1, count, begin, 0)
        local = pltpu.make_async_copy(own, target, sems.at[0, 0])
        local.start()
        lax.fori_loop(1, count, finish, 0)
        local.wait()

    def partner(d):
        return {"gy": other}

    exchange(2, pair_sems, lambda d: spectrum_ref.at[other], both_ref.at[core], partner, spectrum_ref.at[core])
    local_y = both_ref.shape[2]
    total_y = 2 * local_y

    def forward_y(c, carry):
        lines = [both_ref[y // local_y, c, y % local_y] for y in range(total_y)]
        for k in range(total_y):
            total = None
            for y in range(total_y):
                term = float(y_table[k, y]) * lines[y]
                total = term if total is None else total + term
            bands_ref[k, c] = total
        return carry

    lax.fori_loop(0, outer, forward_y, 0)
    exchange(
        inner, inner_sems, lambda d: bands_ref.at[at_col(d)], arrive_ref.at[col],
        lambda d: {"gx": row * inner + at_col(d)}, bands_ref.at[col],
    )
    exchange(
        outer, outer_sems, lambda d: arrive_ref.at[:, at_row(d)], whole_ref.at[row],
        lambda d: {"gx": at_row(d) * inner + col}, arrive_ref.at[:, row],
    )

    shape = whole_ref.shape
    flat = (shape[0] * shape[1] * shape[2], shape[3])

    def transform(value):
        high = value.astype(bf16)
        low = (value - high.astype(f32)).astype(bf16)
        table = high_ref[...]
        return (
            jnp.dot(table, high, preferred_element_type=f32)
            + jnp.dot(table, low, preferred_element_type=f32)
            + jnp.dot(low_ref[...], high, preferred_element_type=f32)
        )

    value = transform(whole_ref[...].reshape(flat)) * weight_ref[...]
    done_ref[...] = transform(value).reshape(shape)

    exchange(
        outer, outer_back_sems, lambda d: done_ref.at[at_row(d)], back_ref.at[:, row],
        lambda d: {"gx": at_row(d) * inner + col}, done_ref.at[row],
    )
    exchange(
        inner, inner_back_sems, lambda d: back_ref.at[at_col(d)], rows_ref.at[col],
        lambda d: {"gx": row * inner + at_col(d)}, back_ref.at[col],
    )

    def inverse_y(c, carry):
        lines = [rows_ref[k, c] for k in range(total_y)]
        for y in range(total_y):
            total = None
            for k in range(total_y):
                term = float(y_table[k, y]) * lines[k]
                total = term if total is None else total + term
            halves_ref[y // local_y, c, y % local_y] = total
        return carry

    lax.fori_loop(0, outer, inverse_y, 0)
    exchange(2, pair_back_sems, lambda d: halves_ref.at[other], out_ref.at[core], partner, halves_ref.at[core])


def filtered_modes(spectrum, weights, x_high, x_low, inner, outer):
    halves, channels, local_y, lines, lanes = spectrum.shape
    band = (channels, lines, lanes)
    scratch = [
        pltpu.VMEM(spectrum.shape, f32),
        pltpu.VMEM((inner,) + band, f32),
        pltpu.VMEM((inner,) + band, f32),
        pltpu.VMEM((outer, inner, lines, lanes), f32),
        pltpu.VMEM((outer, inner, lines, lanes), f32),
        pltpu.VMEM((inner,) + band, f32),
        pltpu.VMEM((inner,) + band, f32),
        pltpu.VMEM(spectrum.shape, f32),
    ]
    sems = [pltpu.SemaphoreType.DMA((2, n)) for n in (2, inner, outer, outer, inner, 2)]
    return pl.pallas_call(
        functools.partial(filter_kernel, inner, outer, hartley(2 * local_y)),
        out_shape=jax.ShapeDtypeStruct(spectrum.shape, f32),
        in_specs=[VMEM] * 4,
        out_specs=VMEM,
        scratch_shapes=scratch + sems,
        compiler_params=pltpu.CompilerParams(collective_id=0, has_side_effects=True, **PARAMS),
        name="filter_modes",
    )(spectrum, weights, x_high, x_low)


def sine_squares(length):
    return np.sin(np.pi * np.arange(length) / length) ** 2


def mode_weights(x_total, y_total, lines):
    sites = NZ * NT
    modes = np.arange(sites)
    plane = sine_squares(NZ)[modes // NT] + sine_squares(NT)[modes % NT]
    plane = jnp.asarray(plane.reshape(2, lines, LANES), f32)[lax.axis_index("gy")]
    y_part = jnp.asarray(sine_squares(y_total), f32)[lax.axis_index("gx") % y_total]
    x_part = jnp.asarray(np.repeat(sine_squares(x_total), lines), f32)
    tiled = jnp.tile(plane, (x_total, 1))
    denom = kernel_mass + 4.0 * (x_part[:, None] + y_part + tiled)
    return (4.0 / (x_total * y_total * sites)) / denom


def shards(gauge_links, momentum):
    channels, _, local_y, sites = momentum.shape
    gx_count = lax.axis_size("gx")
    inner = 2 * local_y
    outer = channels
    lines = sites // LANES // 2
    links = gauge_links.reshape(4, 12, local_y, sites)

    ahead = lax.ppermute(links[1:4], "gx", [((i + 1) % gx_count, i) for i in range(gx_count)])
    bottom_y = links[1, :, local_y - 1]
    edge_rows = jnp.concatenate([links[0, :, 0], links[0, :, local_y - 1], bottom_y])
    edge_rows = lax.ppermute(edge_rows, "gy", [(0, 1), (1, 0)])
    corner = lax.ppermute(
        bottom_y, ("gx", "gy"),
        [(((i + 1) % gx_count) * 2 + 1 - g, i * 2 + g) for i in range(gx_count) for g in range(2)],
    )
    edge_rows = edge_rows.reshape(36, sites // LANES, LANES)
    corner = corner.reshape(12, sites // LANES, LANES)

    plane_high, plane_low = plane_tables()
    weights = mode_weights(gx_count, inner, lines)
    x_high, x_low = in_two(np.kron(hartley(gx_count), np.eye(lines)).astype(np.float32))

    new_momentum, spectrum = pl.pallas_call(
        force_kernel,
        out_shape=[
            jax.ShapeDtypeStruct((channels, local_y, sites), f32),
            jax.ShapeDtypeStruct((2, channels * local_y * lines, LANES), f32),
        ],
        in_specs=[VMEM] * 7,
        out_specs=[VMEM] * 2,
        scratch_shapes=[
            pltpu.VMEM((8, local_y, sites), f32),
            pltpu.VMEM((18, local_y, sites), f32),
            pltpu.VMEM((18, local_y, sites), f32),
            pltpu.VMEM((18, sites // LANES, LANES), f32),
        ],
        compiler_params=pltpu.CompilerParams(**PARAMS),
        name="force_and_plane",
    )(links, ahead, edge_rows, corner, momentum.reshape(channels, local_y, sites), plane_high, plane_low)

    spectrum = spectrum.reshape(2, channels, local_y, lines, LANES)
    filtered = filtered_modes(spectrum, weights, x_high, x_low, inner, outer)
    filtered = filtered.reshape(2, channels * local_y * lines, LANES)

    new_link = pl.pallas_call(
        finish_kernel,
        out_shape=jax.ShapeDtypeStruct((12, local_y, sites), f32),
        in_specs=[VMEM] * 4,
        out_specs=VMEM,
        scratch_shapes=[pltpu.VMEM((channels * local_y, sites), f32)],
        compiler_params=pltpu.CompilerParams(**PARAMS),
        name="link_update",
    )(filtered, links[0], plane_high, plane_low)
    return (new_momentum.reshape(momentum.shape), new_link.reshape(12, 1, local_y, sites))


def solution(mesh):
    return jax.shard_map(
        shards,
        mesh=mesh,
        in_specs=(P(None, None, ("cfg", "gx"), "gy", None), P(None, ("cfg", "gx"), "gy", None)),
        out_specs=(P(None, ("cfg", "gx"), "gy", None), P(None, ("cfg", "gx"), "gy", None)),
        check_vma=False,
    )
```

```python
import functools
import math

import jax
import jax.numpy as jnp
import numpy as np
from jax import lax
from jax.experimental import pallas as pl
from jax.experimental.pallas import tpu as pltpu
from jax.sharding import PartitionSpec as P

NZ = 32
NT = 32
LANES = 128

coupling = 6.0
step_force = 0.3
step_link = 0.15
kernel_mass = 0.01

f32 = jnp.float32
bf16 = jnp.bfloat16
VMEM = pl.BlockSpec(memory_space=pltpu.VMEM)
PARAMS = dict(vmem_limit_bytes=60 * 1024 * 1024)


def hartley(length):
    index = np.arange(length)
    angle = 2.0 * np.pi * (np.outer(index, index) % length) / length
    return np.cos(angle) + np.sin(angle)


def in_two(table):
    high = jnp.asarray(table, f32).astype(bf16)
    return high, (jnp.asarray(table, f32) - high.astype(f32)).astype(bf16)


def cdot(lefts, rights, conj_left=False, conj_right=False):
    re = im = None
    for (a, b), (c, d) in zip(lefts, rights):
        same = conj_left == conj_right
        re_term = a * c - b * d if same else a * c + b * d
        if not conj_left and not conj_right:
            im_term = a * d + b * c
        elif conj_left and not conj_right:
            im_term = a * d - b * c
        elif conj_right and not conj_left:
            im_term = b * c - a * d
        else:
            im_term = -(a * d + b * c)
        re = re_term if re is None else re + re_term
        im = im_term if im is None else im + im_term
    return re, im


def product(left, right, adj_left=False, adj_right=False):
    out = []
    for r in range(3):
        row = []
        lefts = [left[k][r] for k in range(3)] if adj_left else [left[r][k] for k in range(3)]
        for c in range(3):
            rights = [right[c][k] for k in range(3)] if adj_right else [right[k][c] for k in range(3)]
            row.append(cdot(lefts, rights, adj_left, adj_right))
        out.append(row)
    return out


def with_third(rows):
    third = []
    for k in range(3):
        i, j = (k + 1) % 3, (k + 2) % 3
        (a, b), (c, d) = rows[0][i], rows[1][j]
        (e, f), (g, h) = rows[0][j], rows[1][i]
        third.append(((a * c - b * d) - (e * g - f * h), (e * h + f * g) - (a * d + b * c)))
    return [rows[0], rows[1], third]


def matrix_of(get):
    return with_third([[(get(3 * r + k), get(6 + 3 * r + k)) for k in range(3)] for r in range(2)])


def algebra_parts(m):
    inv_root = 1.0 / math.sqrt(3.0)
    return [
        m[1][0][1] + m[0][1][1],
        m[0][1][0] - m[1][0][0],
        m[0][0][1] - m[1][1][1],
        m[2][0][1] + m[0][2][1],
        m[0][2][0] - m[2][0][0],
        m[2][1][1] + m[1][2][1],
        m[1][2][0] - m[2][1][0],
        (m[0][0][1] + m[1][1][1] - 2.0 * m[2][2][1]) * inv_root,
    ]


def split_dot(value, high_ref, low_ref, columns):
    high = value.astype(bf16)
    low = (value - high.astype(f32)).astype(bf16)
    table = high_ref[:, columns]
    return (
        jnp.dot(high, table, preferred_element_type=f32)
        + jnp.dot(low, table, preferred_element_type=f32)
        + jnp.dot(high, low_ref[:, columns], preferred_element_type=f32)
    )


def finish_kernel(smooth_ref, links_ref, momentum_ref, new_ref, copied_ref):
    copied_ref[...] = momentum_ref[...]
    tiles = new_ref.shape[2] // LANES
    root_inv = 1.0 / math.sqrt(3.0)
    scale = 0.25 * step_link * 0.5

    def one(i, carry):
        here = pl.ds(pl.multiple_of(i * LANES, LANES), LANES)
        s = [smooth_ref[pl.ds(8 * a, 8), here] * scale for a in range(8)]
        eighth = root_inv * s[7]
        h00, h11, h22 = eighth + s[2], eighth - s[2], -2.0 * eighth
        a01, b01 = s[0], -s[1]
        a02, b02 = s[3], -s[4]
        a12, b12 = s[5], -s[6]
        n01 = a01 * a01 + b01 * b01
        n02 = a02 * a02 + b02 * b02
        n12 = a12 * a12 + b12 * b12
        p = 0.5 * (h00 * h00 + h11 * h11 + h22 * h22) + (n01 + n02 + n12)
        m_re = a01 * a12 - b01 * b12
        m_im = a01 * b12 + b01 * a12
        q = h00 * h11 * h22 + 2.0 * (m_re * a02 + m_im * b02) - h00 * n12 - h11 * n02 - h22 * n01
        pq = p * q
        pp = p * p
        c0 = (1.0 - q * q * (1.0 / 720.0), pq * (1.0 / 120.0) - q * (1.0 / 6.0))
        c1 = (q * (1.0 / 24.0) - pq * (1.0 / 360.0), 1.0 - p * (1.0 / 6.0) + pp * (1.0 / 120.0))
        c2 = (p * (1.0 / 24.0) - 0.5 - pp * (1.0 / 720.0), q * (1.0 / 120.0))

        def cm(u, v):
            return (u[0] * v[0] - u[1] * v[1], u[0] * v[1] + u[1] * v[0])

        for _ in range(2):
            s00, s11, s22 = cm(c0, c0), cm(c1, c1), cm(c2, c2)
            d01, d02, d12 = cm(c0, c1), cm(c0, c2), cm(c1, c2)
            c0, c1, c2 = (
                tuple(s00[x] + 2.0 * q * d12[x] for x in range(2)),
                tuple(2.0 * (d01[x] + p * d12[x]) + q * s22[x] for x in range(2)),
                tuple(2.0 * d02[x] + s11[x] + p * s22[x] for x in range(2)),
            )
        g00 = h00 * h00 + n01 + n02
        g11 = h11 * h11 + n01 + n12
        g01 = (a01 * (h00 + h11) + a02 * a12 + b02 * b12, b01 * (h00 + h11) + b02 * a12 - a02 * b12)
        g02 = (a02 * (h00 + h22) + m_re, b02 * (h00 + h22) + m_im)
        g12 = (a12 * (h11 + h22) + a01 * a02 + b01 * b02, b12 * (h11 + h22) + a01 * b02 - b01 * a02)

        def mix(h, g):
            first, second = cm(c1, h), cm(c2, g)
            return (first[0] + second[0], first[1] + second[1])

        def diagonal(h, g):
            return (c0[0] + c1[0] * h + c2[0] * g, c0[1] + c1[1] * h + c2[1] * g)

        rotation = [
            [diagonal(h00, g00), mix((a01, b01), g01), mix((a02, b02), g02)],
            [mix((a01, -b01), (g01[0], -g01[1])), diagonal(h11, g11), mix((a12, b12), g12)],
        ]
        link = matrix_of(lambda e: links_ref[0, e, :, here])
        for r in range(2):
            for k in range(3):
                re, im = cdot(rotation[r], [link[m][k] for m in range(3)])
                new_ref[3 * r + k, :, here] = re
                new_ref[6 + 3 * r + k, :, here] = im
        return carry

    lax.fori_loop(0, tiles, one, 0)


def step_kernel(
    inner, outer, y_table,
    links_hbm, momentum_hbm, plane_hbm, modes_hbm, x_hbm, y_squares,
    new_ref, smooth_ref,
    links_ref, ahead_ref, momentum_ref, plane_ref, modes_ref, x_ref,
    high_ref, low_ref, weight_ref, path_ref, partial_ref, staple_ref, behind_ref,
    top_out, top_in, edge_out, edge_in,
    spectrum_ref, both_ref, bands_ref, whole_ref, done_ref, back_ref, halves_ref, filtered_ref,
    load_sems, halo_sems, swap_sems, all_sems, ring_sems,
):
    me = lax.axis_index("gx")
    core = lax.axis_index("gy")
    other = 1 - core
    peers = inner * outer
    row = me // inner
    col = me % inner
    mesh_id = pl.DeviceIdType.MESH
    before = {"gx": lax.rem(me + peers - 1, peers)}
    after = {"gx": lax.rem(me + 1, peers)}
    partner = {"gy": other}
    col_before = {"gx": row * inner + lax.rem(col + inner - 1, inner)}
    col_after = {"gx": row * inner + lax.rem(col + 1, inner)}
    row_before = {"gx": lax.rem(row + outer - 1, outer) * inner + col}
    row_after = {"gx": lax.rem(row + 1, outer) * inner + col}
    neighbours = (before, after, partner, col_before, col_after, row_before, row_after)

    def signal(sem, device):
        pl.semaphore_signal(sem, inc=1, device_id=device, device_id_type=mesh_id)

    def send(source, target, sems, device):
        return pltpu.make_async_remote_copy(
            src_ref=source, dst_ref=target, send_sem=sems.at[0], recv_sem=sems.at[1],
            device_id=device, device_id_type=mesh_id,
        )

    barrier = pltpu.get_barrier_semaphore()
    for device in neighbours:
        signal(barrier, device)
    loads = [
        pltpu.make_async_copy(links_hbm, links_ref, load_sems.at[0]),
        pltpu.make_async_copy(plane_hbm, plane_ref, load_sems.at[1]),
        pltpu.make_async_copy(modes_hbm.at[core], modes_ref, load_sems.at[2]),
        pltpu.make_async_copy(x_hbm, x_ref, load_sems.at[3]),
        pltpu.make_async_copy(momentum_hbm, momentum_ref, load_sems.at[4]),
    ]
    for load in loads:
        load.start()
    pl.semaphore_wait(barrier, len(neighbours))

    halos = [send(links_hbm.at[nu], ahead_ref.at[nu - 1], halo_sems.at[nu - 1], before) for nu in (1, 2, 3)]
    for halo in halos:
        halo.start()

    def relay(steps, behind, ahead, first):
        def step(k, carry):
            signal(ring_sems.at[first], ahead)
            signal(ring_sems.at[first + 1], behind)
            pl.semaphore_wait(ring_sems.at[first], 1)
            pl.semaphore_wait(ring_sems.at[first + 1], 1)
            return carry

        lax.fori_loop(0, steps, step, 0)

    tiles = new_ref.shape[2] // LANES
    lane = lax.broadcasted_iota(jnp.int32, (8, LANES), 1)
    sublane = lax.broadcasted_iota(jnp.int32, (8, LANES), 0)
    t_site = lane % NT

    def lanes_of(i):
        return pl.ds(pl.multiple_of(i * LANES, LANES), LANES)

    loads[0].wait()

    def pack_top(i, carry):
        for e in range(12):
            top_out[e, pl.ds(i, 1), :] = links_ref[0, e, 0:1, lanes_of(i)]
        return carry

    lax.fori_loop(0, tiles, pack_top, 0)
    top = send(top_out, top_in, halo_sems.at[3], partner)
    top.start()
    relay(inner // 2, col_before, col_after, 0)
    relay(outer // 2, row_before, row_after, 2)

    for load in loads[1:]:
        load.wait()

    def table_block(z, carry):
        full = plane_ref[0] * plane_ref[1, pl.ds(z, 1), :]
        high = full.astype(bf16)
        rows = pl.ds(pl.multiple_of(z * NT, NT), NT)
        high_ref[rows, :] = high
        low_ref[rows, :] = (full - high.astype(f32)).astype(bf16)
        return carry

    lax.fori_loop(0, NZ, table_block, 0)
    scale = 4.0 / (peers * inner * NZ * NT)
    weight_ref[...] = scale / (kernel_mass + 4.0 * (modes_ref[...] + y_squares[col]))
    top.wait()

    def prepare(i, carry):
        here = lanes_of(i)
        following = lanes_of(lax.rem(i + 1, tiles))

        def moved_y(e):
            edge = jnp.broadcast_to(top_in[e, pl.ds(i, 1), :], (8, LANES))
            return jnp.where(sublane == 7, edge, pltpu.roll(links_ref[0, e, :, here], 7, 0))

        def moved_z(e):
            return jnp.where(
                lane < LANES - NT,
                pltpu.roll(links_ref[0, e, :, here], LANES - NT, 1),
                pltpu.roll(links_ref[0, e, :, following], LANES - NT, 1),
            )

        def moved_t(e):
            value = links_ref[0, e, :, here]
            return jnp.where(
                t_site == NT - 1, pltpu.roll(value, NT - 1, 1), pltpu.roll(value, LANES - 1, 1)
            )

        for nu, moved in ((1, moved_y), (2, moved_z), (3, moved_t)):
            link_nu = matrix_of(lambda e: links_ref[nu, e, :, here])
            path = product(link_nu, matrix_of(moved))
            for r in range(3):
                for k in range(3):
                    path_ref[nu - 1, 3 * r + k, :, here] = path[r][k][0]
                    path_ref[nu - 1, 9 + 3 * r + k, :, here] = path[r][k][1]
        return carry

    lax.fori_loop(0, tiles, prepare, 0)

    def staples(nu, i):
        here = lanes_of(i)
        link_x = matrix_of(lambda e: links_ref[0, e, :, here])
        link_nu = matrix_of(lambda e: links_ref[nu, e, :, here])
        ahead = matrix_of(lambda e: ahead_ref[nu - 1, e, :, here])
        corner = product(link_x, ahead)
        lower = product(corner, link_nu, adj_left=True)
        path = [
            [(path_ref[nu - 1, 3 * r + k, :, here], path_ref[nu - 1, 9 + 3 * r + k, :, here]) for k in range(3)]
            for r in range(3)
        ]
        parts = algebra_parts(product(corner, path, adj_right=True))
        for a in range(8):
            if nu == 1:
                partial_ref[a, :, here] = parts[a]
            else:
                partial_ref[a, :, here] += parts[a]
        return here, [lower[r][k][p] for p in range(2) for r in range(3) for k in range(3)]

    def along_y(i, carry):
        here, flat = staples(1, i)
        for e in range(18):
            edge_out[e, pl.ds(i, 1), :] = flat[e][7:8, :]
            staple_ref[e, :, here] = jnp.where(sublane == 0, 0.0, pltpu.roll(flat[e], 1, 0))
        return carry

    def along_z(i, carry):
        here, flat = staples(2, i)
        for e in range(18):
            behind_ref[e, :, here] = flat[e]
        return carry

    def along_t(i, carry):
        here, flat = staples(3, i)
        for e in range(18):
            staple_ref[e, :, here] += jnp.where(
                t_site == 0, pltpu.roll(flat[e], LANES - NT + 1, 1), pltpu.roll(flat[e], 1, 1)
            )
        return carry

    halos[0].wait_recv()
    lax.fori_loop(0, tiles, along_y, 0)
    edge = send(edge_out, edge_in, halo_sems.at[4], partner)
    edge.start()
    halos[1].wait_recv()
    lax.fori_loop(0, tiles, along_z, 0)
    halos[2].wait_recv()
    lax.fori_loop(0, tiles, along_t, 0)
    edge.wait()

    def force(i, carry):
        here = lanes_of(i)
        previous = lanes_of(lax.rem(i + tiles - 1, tiles))
        flat = [
            staple_ref[e, :, here]
            + jnp.where(sublane == 0, jnp.broadcast_to(edge_in[e, pl.ds(i, 1), :], (8, LANES)), 0.0)
            + jnp.where(
                lane >= NT,
                pltpu.roll(behind_ref[e, :, here], NT, 1),
                pltpu.roll(behind_ref[e, :, previous], NT, 1),
            )
            for e in range(18)
        ]
        staple = [[(flat[3 * r + k], flat[9 + 3 * r + k]) for k in range(3)] for r in range(3)]
        link_x = matrix_of(lambda e: links_ref[0, e, :, here])
        parts = algebra_parts(product(link_x, staple))
        for a in range(8):
            total = (coupling / 6.0) * (partial_ref[a, :, here] + parts[a])
            new_ref[a, :, here] = momentum_ref[a, :, here] - step_force * total
        return carry

    lax.fori_loop(0, tiles, force, 0)

    count = new_ref.shape[0] * new_ref.shape[1]
    half = tiles // 2
    value = new_ref[...].reshape(count, tiles * LANES)
    for pair in range(half):
        columns = slice(pair * 2 * LANES, (pair + 1) * 2 * LANES)
        out = split_dot(value, high_ref, low_ref, columns)
        for side in range(2):
            tile = 2 * pair + side
            spectrum_ref[tile // half, pl.ds(tile % half, count, stride=half), :] = out[
                :, side * LANES : (side + 1) * LANES
            ]

    def swap(source, target, stage):
        remote = send(source.at[other], target.at[core], swap_sems.at[stage], partner)
        remote.start()
        local = pltpu.make_async_copy(source.at[core], target.at[core], swap_sems.at[stage, 2])
        local.start()
        local.wait()
        remote.wait()

    def peer(d):
        step = (d + 1) // 2
        return lax.rem(me + lax.select(lax.rem(d, 2) == 1, step, peers - step), peers)

    def all_to_all(source, target, stage):
        def begin(d, carry):
            to = peer(d)
            send(source.at[to], target.at[me], all_sems.at[stage], {"gx": to}).start()
            return carry

        lax.fori_loop(1, peers, begin, 0)
        local = pltpu.make_async_copy(source.at[me], target.at[me], all_sems.at[stage, 2])
        local.start()
        local.wait()
        rest = pl.ds(0, peers - 1)
        pltpu.make_async_copy(source.at[rest], source.at[rest], all_sems.at[stage, 0]).wait()
        pltpu.make_async_copy(target.at[rest], target.at[rest], all_sems.at[stage, 1]).wait()

    swap(spectrum_ref, both_ref, 0)
    local_y = new_ref.shape[1]
    total_y = 2 * local_y

    def lines_of(c, y):
        return pl.ds(pl.multiple_of(c * (local_y * half), local_y * half) + (y % local_y) * half, half)

    def forward_y(c, carry):
        lines = [both_ref[y // local_y, lines_of(c, y), :] for y in range(total_y)]
        for k in range(total_y):
            total = None
            for y in range(total_y):
                term = float(y_table[k, y]) * lines[y]
                total = term if total is None else total + term
            bands_ref[c * inner + k] = total
        return carry

    lax.fori_loop(0, outer, forward_y, 0)
    all_to_all(bands_ref, whole_ref, 0)

    shape = whole_ref.shape
    flat_shape = (shape[0] * shape[1], shape[2])

    def transform(value):
        high = value.astype(bf16)
        low = (value - high.astype(f32)).astype(bf16)
        table = x_ref[0]
        return (
            jnp.dot(table, high, preferred_element_type=f32)
            + jnp.dot(table, low, preferred_element_type=f32)
            + jnp.dot(x_ref[1], high, preferred_element_type=f32)
        )

    modes = transform(whole_ref[...].reshape(flat_shape)) * weight_ref[...]
    done_ref[...] = transform(modes).reshape(shape)
    all_to_all(done_ref, back_ref, 1)

    def inverse_y(c, carry):
        lines = [back_ref[c * inner + k] for k in range(total_y)]
        for y in range(total_y):
            total = None
            for k in range(total_y):
                term = float(y_table[k, y]) * lines[k]
                total = term if total is None else total + term
            halves_ref[y // local_y, lines_of(c, y), :] = total
        return carry

    lax.fori_loop(0, outer, inverse_y, 0)
    swap(halves_ref, filtered_ref, 1)
    value = jnp.concatenate(
        [filtered_ref[tile // half, pl.ds(tile % half, count, stride=half), :] for tile in range(tiles)],
        axis=1,
    )
    for pair in range(half):
        columns = slice(pair * 2 * LANES, (pair + 1) * 2 * LANES)
        smooth_ref[:, columns] = split_dot(value, high_ref, low_ref, columns)
    for halo in halos:
        halo.wait_send()


def sine_squares(length):
    return np.sin(np.pi * np.arange(length) / length) ** 2


def shards(gauge_links, momentum):
    channels, _, local_y, sites = momentum.shape
    gx_count = lax.axis_size("gx")
    inner = 2 * local_y
    outer = channels
    tiles = sites // LANES
    half = tiles // 2
    rows = channels * local_y
    links = gauge_links.reshape(4, 12, local_y, sites)
    field = (channels, local_y, sites)

    plane = np.stack([np.tile(hartley(NT), (1, NZ)), np.repeat(hartley(NZ), NT, axis=1)]).astype(np.float32)
    index = np.arange(sites)
    z_t = (sine_squares(NZ)[index // NT] + sine_squares(NT)[index % NT]).reshape(2, half, LANES)
    modes = np.tile(z_t, (1, gx_count, 1)) + np.repeat(sine_squares(gx_count), half)[None, :, None]
    x_high, x_low = in_two(np.kron(hartley(gx_count), np.eye(half)).astype(np.float32))
    x_table = jnp.stack([x_high, x_low])
    y_squares = jnp.asarray(sine_squares(inner), f32)

    any_spec = pl.BlockSpec(memory_space=pl.ANY)
    exchanged = (gx_count, half, LANES)
    halved = (2, rows * half, LANES)
    staple = (18, local_y, sites)
    new_momentum, smooth = pl.pallas_call(
        functools.partial(step_kernel, inner, outer, hartley(inner)),
        out_shape=[jax.ShapeDtypeStruct(field, f32), jax.ShapeDtypeStruct((rows, sites), f32)],
        in_specs=[any_spec] * 5 + [pl.BlockSpec(memory_space=pltpu.SMEM)],
        out_specs=[VMEM] * 2,
        scratch_shapes=[
            pltpu.VMEM(links.shape, f32),
            pltpu.VMEM((3,) + links.shape[1:], f32),
            pltpu.VMEM(field, f32),
            pltpu.VMEM(plane.shape, f32),
            pltpu.VMEM(modes.shape[1:], f32),
            pltpu.VMEM(x_table.shape, bf16),
            pltpu.VMEM((sites, sites), bf16),
            pltpu.VMEM((sites, sites), bf16),
            pltpu.VMEM(modes.shape[1:], f32),
            pltpu.VMEM((3,) + staple, f32),
            pltpu.VMEM(field, f32),
            pltpu.VMEM(staple, f32),
            pltpu.VMEM(staple, f32),
            pltpu.VMEM((12, tiles, LANES), f32),
            pltpu.VMEM((12, tiles, LANES), f32),
            pltpu.VMEM((18, tiles, LANES), f32),
            pltpu.VMEM((18, tiles, LANES), f32),
            pltpu.VMEM(halved, f32),
            pltpu.VMEM(halved, f32),
            pltpu.VMEM(exchanged, f32),
            pltpu.VMEM(exchanged, f32),
            pltpu.VMEM(exchanged, f32),
            pltpu.VMEM(exchanged, f32),
            pltpu.VMEM(halved, f32),
            pltpu.VMEM(halved, f32),
            pltpu.SemaphoreType.DMA((5,)),
            pltpu.SemaphoreType.DMA((5, 2)),
            pltpu.SemaphoreType.DMA((2, 3)),
            pltpu.SemaphoreType.DMA((2, 3)),
            pltpu.SemaphoreType.REGULAR((4,)),
        ],
        compiler_params=pltpu.CompilerParams(collective_id=0, has_side_effects=True, **PARAMS),
        name="momentum_and_smooth",
    )(links, momentum.reshape(field), jnp.asarray(plane), jnp.asarray(modes, f32), x_table, y_squares)

    width = 2 * LANES
    new_link, new_momentum = pl.pallas_call(
        finish_kernel,
        grid=(sites // width,),
        out_shape=[jax.ShapeDtypeStruct(links.shape[1:], f32), jax.ShapeDtypeStruct(field, f32)],
        in_specs=[
            pl.BlockSpec((rows, width), lambda i: (0, i)),
            pl.BlockSpec((1, 12, local_y, width), lambda i: (0, 0, 0, i)),
            pl.BlockSpec((channels, local_y, width), lambda i: (0, 0, i)),
        ],
        out_specs=[
            pl.BlockSpec((12, local_y, width), lambda i: (0, 0, i)),
            pl.BlockSpec((channels, local_y, width), lambda i: (0, 0, i)),
        ],
        compiler_params=pltpu.CompilerParams(**PARAMS),
        name="link_update",
    )(smooth, links, new_momentum)
    return (new_momentum.reshape(momentum.shape), new_link.reshape(12, 1, local_y, sites))


def solution(mesh):
    return jax.shard_map(
        shards,
        mesh=mesh,
        in_specs=(P(None, None, ("cfg", "gx"), "gy", None), P(None, ("cfg", "gx"), "gy", None)),
        out_specs=(P(None, ("cfg", "gx"), "gy", None), P(None, ("cfg", "gx"), "gy", None)),
        check_vma=False,
    )
```

```python
import functools
import math

import jax
import jax.numpy as jnp
import numpy as np
from jax import lax
from jax.experimental import pallas as pl
from jax.experimental.pallas import tpu as pltpu
from jax.sharding import PartitionSpec as P

NZ = 32
NT = 32
LANES = 128

coupling = 6.0
step_force = 0.3
step_link = 0.15
kernel_mass = 0.01

f32 = jnp.float32
bf16 = jnp.bfloat16
VMEM = pl.BlockSpec(memory_space=pltpu.VMEM)
PARAMS = dict(vmem_limit_bytes=60 * 1024 * 1024)


def hartley(length):
    index = np.arange(length)
    angle = 2.0 * np.pi * (np.outer(index, index) % length) / length
    return np.cos(angle) + np.sin(angle)


def in_two(table):
    high = jnp.asarray(table, f32).astype(bf16)
    return high, (jnp.asarray(table, f32) - high.astype(f32)).astype(bf16)


def cdot(lefts, rights, conj_left=False, conj_right=False):
    re = im = None
    for (a, b), (c, d) in zip(lefts, rights):
        same = conj_left == conj_right
        re_term = a * c - b * d if same else a * c + b * d
        if not conj_left and not conj_right:
            im_term = a * d + b * c
        elif conj_left and not conj_right:
            im_term = a * d - b * c
        elif conj_right and not conj_left:
            im_term = b * c - a * d
        else:
            im_term = -(a * d + b * c)
        re = re_term if re is None else re + re_term
        im = im_term if im is None else im + im_term
    return re, im


def product(left, right, adj_left=False, adj_right=False):
    out = []
    for r in range(3):
        row = []
        lefts = [left[k][r] for k in range(3)] if adj_left else [left[r][k] for k in range(3)]
        for c in range(3):
            rights = [right[c][k] for k in range(3)] if adj_right else [right[k][c] for k in range(3)]
            row.append(cdot(lefts, rights, adj_left, adj_right))
        out.append(row)
    return out


def with_third(rows):
    third = []
    for k in range(3):
        i, j = (k + 1) % 3, (k + 2) % 3
        (a, b), (c, d) = rows[0][i], rows[1][j]
        (e, f), (g, h) = rows[0][j], rows[1][i]
        third.append(((a * c - b * d) - (e * g - f * h), (e * h + f * g) - (a * d + b * c)))
    return [rows[0], rows[1], third]


def matrix_of(get):
    return with_third([[(get(3 * r + k), get(6 + 3 * r + k)) for k in range(3)] for r in range(2)])


def algebra_parts(m):
    inv_root = 1.0 / math.sqrt(3.0)
    return [
        m[1][0][1] + m[0][1][1],
        m[0][1][0] - m[1][0][0],
        m[0][0][1] - m[1][1][1],
        m[2][0][1] + m[0][2][1],
        m[0][2][0] - m[2][0][0],
        m[2][1][1] + m[1][2][1],
        m[1][2][0] - m[2][1][0],
        (m[0][0][1] + m[1][1][1] - 2.0 * m[2][2][1]) * inv_root,
    ]


def split_dot(value, high_ref, low_ref, columns, rows=slice(None)):
    high = value.astype(bf16)
    low = (value - high.astype(f32)).astype(bf16)
    table = high_ref[rows, columns]
    return (
        jnp.dot(high, table, preferred_element_type=f32)
        + jnp.dot(low, table, preferred_element_type=f32)
        + jnp.dot(high, low_ref[rows, columns], preferred_element_type=f32)
    )


def finish_kernel(smooth_ref, links_ref, momentum_ref, new_ref, copied_ref):
    copied_ref[...] = momentum_ref[...]
    tiles = new_ref.shape[2] // LANES
    root_inv = 1.0 / math.sqrt(3.0)
    scale = 0.25 * step_link * 0.5

    def one(i, carry):
        here = pl.ds(pl.multiple_of(i * LANES, LANES), LANES)
        s = [smooth_ref[pl.ds(8 * a, 8), here] * scale for a in range(8)]
        eighth = root_inv * s[7]
        h00, h11, h22 = eighth + s[2], eighth - s[2], -2.0 * eighth
        a01, b01 = s[0], -s[1]
        a02, b02 = s[3], -s[4]
        a12, b12 = s[5], -s[6]
        n01 = a01 * a01 + b01 * b01
        n02 = a02 * a02 + b02 * b02
        n12 = a12 * a12 + b12 * b12
        p = 0.5 * (h00 * h00 + h11 * h11 + h22 * h22) + (n01 + n02 + n12)
        m_re = a01 * a12 - b01 * b12
        m_im = a01 * b12 + b01 * a12
        q = h00 * h11 * h22 + 2.0 * (m_re * a02 + m_im * b02) - h00 * n12 - h11 * n02 - h22 * n01
        pq = p * q
        pp = p * p
        c0 = (1.0 - q * q * (1.0 / 720.0), pq * (1.0 / 120.0) - q * (1.0 / 6.0))
        c1 = (q * (1.0 / 24.0) - pq * (1.0 / 360.0), 1.0 - p * (1.0 / 6.0) + pp * (1.0 / 120.0))
        c2 = (p * (1.0 / 24.0) - 0.5 - pp * (1.0 / 720.0), q * (1.0 / 120.0))

        def cm(u, v):
            return (u[0] * v[0] - u[1] * v[1], u[0] * v[1] + u[1] * v[0])

        for _ in range(2):
            s00, s11, s22 = cm(c0, c0), cm(c1, c1), cm(c2, c2)
            d01, d02, d12 = cm(c0, c1), cm(c0, c2), cm(c1, c2)
            c0, c1, c2 = (
                tuple(s00[x] + 2.0 * q * d12[x] for x in range(2)),
                tuple(2.0 * (d01[x] + p * d12[x]) + q * s22[x] for x in range(2)),
                tuple(2.0 * d02[x] + s11[x] + p * s22[x] for x in range(2)),
            )
        g00 = h00 * h00 + n01 + n02
        g11 = h11 * h11 + n01 + n12
        g01 = (a01 * (h00 + h11) + a02 * a12 + b02 * b12, b01 * (h00 + h11) + b02 * a12 - a02 * b12)
        g02 = (a02 * (h00 + h22) + m_re, b02 * (h00 + h22) + m_im)
        g12 = (a12 * (h11 + h22) + a01 * a02 + b01 * b02, b12 * (h11 + h22) + a01 * b02 - b01 * a02)

        def mix(h, g):
            first, second = cm(c1, h), cm(c2, g)
            return (first[0] + second[0], first[1] + second[1])

        def diagonal(h, g):
            return (c0[0] + c1[0] * h + c2[0] * g, c0[1] + c1[1] * h + c2[1] * g)

        rotation = [
            [diagonal(h00, g00), mix((a01, b01), g01), mix((a02, b02), g02)],
            [mix((a01, -b01), (g01[0], -g01[1])), diagonal(h11, g11), mix((a12, b12), g12)],
        ]
        link = matrix_of(lambda e: links_ref[0, e, :, here])
        for r in range(2):
            for k in range(3):
                re, im = cdot(rotation[r], [link[m][k] for m in range(3)])
                new_ref[3 * r + k, :, here] = re
                new_ref[6 + 3 * r + k, :, here] = im
        return carry

    lax.fori_loop(0, tiles, one, 0)


def step_kernel(
    inner, outer, y_table,
    links_hbm, momentum_hbm, plane_hbm, modes_hbm, x_hbm, y_squares,
    new_ref, smooth_ref,
    links_ref, ahead_ref, momentum_ref, plane_ref, modes_ref, x_ref,
    high_ref, low_ref, weight_ref, path_ref, partial_ref, staple_ref, behind_ref,
    top_out, top_in, edge_out, edge_in,
    plane_sum_ref, spectrum_ref, both_ref, bands_ref, whole_ref, done_ref, back_ref, halves_ref, filtered_ref,
    load_sems, halo_sems, swap_sems, all_sems, ring_sems,
):
    me = lax.axis_index("gx")
    core = lax.axis_index("gy")
    other = 1 - core
    peers = inner * outer
    row = me // inner
    col = me % inner
    mesh_id = pl.DeviceIdType.MESH
    part = lax.axis_index("cfg")

    def wrapped(value, count):
        return lax.select(value >= count, value - count, value)

    def at(place):
        return (part, place, core)

    def in_row(step):
        return at(row * inner + wrapped(col + step % inner, inner))

    def in_column(step):
        return at(wrapped(row + step % outer, outer) * inner + col)

    before = at(wrapped(me + peers - 1, peers))
    after = at(wrapped(me + 1, peers))
    partner = (part, me, other)
    col_before, col_after = in_row(-1), in_row(1)
    row_before, row_after = in_column(-1), in_column(1)
    neighbours = (before, after, partner, col_before, col_after, row_before, row_after)

    def signal(sem, device):
        pl.semaphore_signal(sem, inc=1, device_id=device, device_id_type=mesh_id)

    def send(source, target, sems, device):
        return pltpu.make_async_remote_copy(
            src_ref=source, dst_ref=target, send_sem=sems.at[0], recv_sem=sems.at[1],
            device_id=device, device_id_type=mesh_id,
        )

    barrier = pltpu.get_barrier_semaphore()
    for device in neighbours:
        signal(barrier, device)
    loads = [
        pltpu.make_async_copy(links_hbm, links_ref, load_sems.at[0]),
        pltpu.make_async_copy(plane_hbm, plane_ref, load_sems.at[1]),
        pltpu.make_async_copy(modes_hbm.at[core], modes_ref, load_sems.at[2]),
        pltpu.make_async_copy(x_hbm, x_ref, load_sems.at[3]),
        pltpu.make_async_copy(momentum_hbm, momentum_ref, load_sems.at[4]),
    ]
    for load in loads:
        load.start()
    pl.semaphore_wait(barrier, len(neighbours))

    sites = new_ref.shape[2]
    halos = [send(links_hbm.at[nu], ahead_ref.at[nu - 1], halo_sems.at[nu - 1], before) for nu in (1, 2)]
    quarters = 4
    width = sites // quarters
    for q in range(quarters):
        lanes = pl.ds(q * width, width)
        halos.append(
            send(links_hbm.at[3, :, :, lanes], ahead_ref.at[2, :, :, lanes], halo_sems.at[2 + q], before)
        )
    for halo in halos:
        halo.start()

    def relay(count, known, place, stage):
        while known < count // 2:
            distance = max(known, 1)
            signal(ring_sems.at[stage], place(distance))
            signal(ring_sems.at[stage], place(-distance))
            pl.semaphore_wait(ring_sems.at[stage], 2)
            known += distance
            stage += 1
        return stage

    tiles = new_ref.shape[2] // LANES
    lane = lax.broadcasted_iota(jnp.int32, (8, LANES), 1)
    sublane = lax.broadcasted_iota(jnp.int32, (8, LANES), 0)
    t_site = lane % NT

    def lanes_of(i):
        return pl.ds(pl.multiple_of(i * LANES, LANES), LANES)

    loads[0].wait()

    def pack_top(i, carry):
        for e in range(12):
            top_out[e, pl.ds(i, 1), :] = links_ref[0, e, 0:1, lanes_of(i)]
        return carry

    lax.fori_loop(0, tiles, pack_top, 0)
    top = send(top_out, top_in, halo_sems.at[2 + quarters], partner)
    top.start()

    for load in loads[1:]:
        load.wait()

    def table_block(z, carry):
        full = plane_ref[0] * plane_ref[1, pl.ds(z, 1), :]
        high = full.astype(bf16)
        rows = pl.ds(pl.multiple_of(z * NT, NT), NT)
        high_ref[rows, :] = high
        low_ref[rows, :] = (full - high.astype(f32)).astype(bf16)
        return carry

    lax.fori_loop(0, NZ, table_block, 0)
    scale = 4.0 / (peers * inner * NZ * NT)
    weight_ref[...] = scale / (kernel_mass + 4.0 * (modes_ref[...] + y_squares[col]))
    last = relay(inner, 1, in_row, 0)
    relay(outer, 0, in_column, last)
    top.wait()

    def prepare(i, carry):
        here = lanes_of(i)
        following = lanes_of(lax.rem(i + 1, tiles))

        def moved_y(e):
            edge = jnp.broadcast_to(top_in[e, pl.ds(i, 1), :], (8, LANES))
            return jnp.where(sublane == 7, edge, pltpu.roll(links_ref[0, e, :, here], 7, 0))

        def moved_z(e):
            return jnp.where(
                lane < LANES - NT,
                pltpu.roll(links_ref[0, e, :, here], LANES - NT, 1),
                pltpu.roll(links_ref[0, e, :, following], LANES - NT, 1),
            )

        def moved_t(e):
            value = links_ref[0, e, :, here]
            return jnp.where(
                t_site == NT - 1, pltpu.roll(value, NT - 1, 1), pltpu.roll(value, LANES - 1, 1)
            )

        for nu, moved in ((1, moved_y), (2, moved_z), (3, moved_t)):
            link_nu = matrix_of(lambda e: links_ref[nu, e, :, here])
            path = product(link_nu, matrix_of(moved))
            for r in range(3):
                for k in range(3):
                    path_ref[nu - 1, 3 * r + k, :, here] = path[r][k][0]
                    path_ref[nu - 1, 9 + 3 * r + k, :, here] = path[r][k][1]
        return carry

    lax.fori_loop(0, tiles, prepare, 0)

    def staples(nu, i):
        here = lanes_of(i)
        link_x = matrix_of(lambda e: links_ref[0, e, :, here])
        link_nu = matrix_of(lambda e: links_ref[nu, e, :, here])
        ahead = matrix_of(lambda e: ahead_ref[nu - 1, e, :, here])
        corner = product(link_x, ahead)
        lower = product(corner, link_nu, adj_left=True)
        path = [
            [(path_ref[nu - 1, 3 * r + k, :, here], path_ref[nu - 1, 9 + 3 * r + k, :, here]) for k in range(3)]
            for r in range(3)
        ]
        parts = algebra_parts(product(corner, path, adj_right=True))
        for a in range(8):
            if nu == 1:
                partial_ref[a, :, here] = parts[a]
            else:
                partial_ref[a, :, here] += parts[a]
        return here, [lower[r][k][p] for p in range(2) for r in range(3) for k in range(3)]

    def along_y(i, carry):
        here, flat = staples(1, i)
        for e in range(18):
            edge_out[e, pl.ds(i, 1), :] = flat[e][7:8, :]
            staple_ref[e, :, here] = jnp.where(sublane == 0, 0.0, pltpu.roll(flat[e], 1, 0))
        return carry

    def along_z(i, carry):
        here, flat = staples(2, i)
        for e in range(18):
            behind_ref[e, :, here] = flat[e]
        return carry

    def along_t(i, carry):
        here, flat = staples(3, i)
        for e in range(18):
            staple_ref[e, :, here] += jnp.where(
                t_site == 0, pltpu.roll(flat[e], LANES - NT + 1, 1), pltpu.roll(flat[e], 1, 1)
            )
        return carry

    halos[0].wait_recv()
    lax.fori_loop(0, tiles, along_y, 0)
    edge = send(edge_out, edge_in, halo_sems.at[3 + quarters], partner)
    edge.start()
    halos[1].wait_recv()
    lax.fori_loop(0, tiles, along_z, 0)
    edge.wait()

    def force(i, carry):
        here = lanes_of(i)
        previous = lanes_of(lax.rem(i + tiles - 1, tiles))
        flat = [
            staple_ref[e, :, here]
            + jnp.where(sublane == 0, jnp.broadcast_to(edge_in[e, pl.ds(i, 1), :], (8, LANES)), 0.0)
            + jnp.where(
                lane >= NT,
                pltpu.roll(behind_ref[e, :, here], NT, 1),
                pltpu.roll(behind_ref[e, :, previous], NT, 1),
            )
            for e in range(18)
        ]
        staple = [[(flat[3 * r + k], flat[9 + 3 * r + k]) for k in range(3)] for r in range(3)]
        link_x = matrix_of(lambda e: links_ref[0, e, :, here])
        parts = algebra_parts(product(link_x, staple))
        for a in range(8):
            total = (coupling / 6.0) * (partial_ref[a, :, here] + parts[a])
            new_ref[a, :, here] = momentum_ref[a, :, here] - step_force * total
        return carry

    count = new_ref.shape[0] * new_ref.shape[1]
    half = tiles // 2
    per = tiles // quarters
    for q in range(quarters):
        halos[2 + q].wait_recv()
        lax.fori_loop(per * q, per * (q + 1), along_t, 0)
        lax.fori_loop(per * q, per * (q + 1), force, 0)
        taken = slice(q * width, (q + 1) * width)
        value = new_ref[:, :, taken].reshape(count, width)
        for pair in range(half):
            columns = slice(pair * 2 * LANES, (pair + 1) * 2 * LANES)
            out = split_dot(value, high_ref, low_ref, columns, taken)
            if q:
                out = out + plane_sum_ref[:, columns]
            if q < quarters - 1:
                plane_sum_ref[:, columns] = out
                continue
            for side in range(2):
                tile = 2 * pair + side
                spectrum_ref[tile // half, pl.ds(tile % half, count, stride=half), :] = out[
                    :, side * LANES : (side + 1) * LANES
                ]

    def swap(source, target, stage):
        remote = send(source.at[other], target.at[core], swap_sems.at[stage], partner)
        remote.start()
        local = pltpu.make_async_copy(source.at[core], target.at[core], swap_sems.at[stage, 2])
        local.start()
        local.wait()
        remote.wait()

    def all_to_all(source, target, stage):
        def push(to):
            send(source.at[to], target.at[me], all_sems.at[stage], at(to)).start()

        def begin(d, carry):
            push(wrapped(me + d, peers))
            push(wrapped(me + peers - d, peers))
            return carry

        lax.fori_loop(1, peers // 2, begin, 0)
        push(wrapped(me + peers // 2, peers))
        local = pltpu.make_async_copy(source.at[me], target.at[me], all_sems.at[stage, 2])
        local.start()
        local.wait()
        rest = pl.ds(0, peers - 1)
        pltpu.make_async_copy(source.at[rest], source.at[rest], all_sems.at[stage, 0]).wait()
        pltpu.make_async_copy(target.at[rest], target.at[rest], all_sems.at[stage, 1]).wait()

    swap(spectrum_ref, both_ref, 0)
    local_y = new_ref.shape[1]
    total_y = 2 * local_y

    def lines_of(c, y):
        return pl.ds(pl.multiple_of(c * (local_y * half), local_y * half) + (y % local_y) * half, half)

    def forward_y(c, carry):
        lines = [both_ref[y // local_y, lines_of(c, y), :] for y in range(total_y)]
        for k in range(total_y):
            total = None
            for y in range(total_y):
                term = float(y_table[k, y]) * lines[y]
                total = term if total is None else total + term
            bands_ref[c * inner + k] = total
        return carry

    lax.fori_loop(0, outer, forward_y, 0)
    all_to_all(bands_ref, whole_ref, 0)

    shape = whole_ref.shape
    flat_shape = (shape[0] * shape[1], shape[2])

    def transform(value):
        high = value.astype(bf16)
        low = (value - high.astype(f32)).astype(bf16)
        table = x_ref[0]
        return (
            jnp.dot(table, high, preferred_element_type=f32)
            + jnp.dot(table, low, preferred_element_type=f32)
            + jnp.dot(x_ref[1], high, preferred_element_type=f32)
        )

    modes = transform(whole_ref[...].reshape(flat_shape)) * weight_ref[...]
    done_ref[...] = transform(modes).reshape(shape)
    all_to_all(done_ref, back_ref, 1)

    def inverse_y(c, carry):
        lines = [back_ref[c * inner + k] for k in range(total_y)]
        for y in range(total_y):
            total = None
            for k in range(total_y):
                term = float(y_table[k, y]) * lines[k]
                total = term if total is None else total + term
            halves_ref[y // local_y, lines_of(c, y), :] = total
        return carry

    lax.fori_loop(0, outer, inverse_y, 0)
    swap(halves_ref, filtered_ref, 1)
    value = jnp.concatenate(
        [filtered_ref[tile // half, pl.ds(tile % half, count, stride=half), :] for tile in range(tiles)],
        axis=1,
    )
    for pair in range(half):
        columns = slice(pair * 2 * LANES, (pair + 1) * 2 * LANES)
        smooth_ref[:, columns] = split_dot(value, high_ref, low_ref, columns)
    for halo in halos:
        halo.wait_send()


def sine_squares(length):
    return np.sin(np.pi * np.arange(length) / length) ** 2


def shards(gauge_links, momentum):
    channels, _, local_y, sites = momentum.shape
    gx_count = lax.axis_size("gx")
    inner = 2 * local_y
    outer = channels
    tiles = sites // LANES
    half = tiles // 2
    rows = channels * local_y
    links = gauge_links.reshape(4, 12, local_y, sites)
    field = (channels, local_y, sites)

    plane = np.stack([np.tile(hartley(NT), (1, NZ)), np.repeat(hartley(NZ), NT, axis=1)]).astype(np.float32)
    index = np.arange(sites)
    z_t = (sine_squares(NZ)[index // NT] + sine_squares(NT)[index % NT]).reshape(2, half, LANES)
    modes = np.tile(z_t, (1, gx_count, 1)) + np.repeat(sine_squares(gx_count), half)[None, :, None]
    x_high, x_low = in_two(np.kron(hartley(gx_count), np.eye(half)).astype(np.float32))
    x_table = jnp.stack([x_high, x_low])
    y_squares = jnp.asarray(sine_squares(inner), f32)

    any_spec = pl.BlockSpec(memory_space=pl.ANY)
    exchanged = (gx_count, half, LANES)
    halved = (2, rows * half, LANES)
    staple = (18, local_y, sites)
    new_momentum, smooth = pl.pallas_call(
        functools.partial(step_kernel, inner, outer, hartley(inner)),
        out_shape=[jax.ShapeDtypeStruct(field, f32), jax.ShapeDtypeStruct((rows, sites), f32)],
        in_specs=[any_spec] * 5 + [pl.BlockSpec(memory_space=pltpu.SMEM)],
        out_specs=[VMEM] * 2,
        scratch_shapes=[
            pltpu.VMEM(links.shape, f32),
            pltpu.VMEM((3,) + links.shape[1:], f32),
            pltpu.VMEM(field, f32),
            pltpu.VMEM(plane.shape, f32),
            pltpu.VMEM(modes.shape[1:], f32),
            pltpu.VMEM(x_table.shape, bf16),
            pltpu.VMEM((sites, sites), bf16),
            pltpu.VMEM((sites, sites), bf16),
            pltpu.VMEM(modes.shape[1:], f32),
            pltpu.VMEM((3,) + staple, f32),
            pltpu.VMEM(field, f32),
            pltpu.VMEM(staple, f32),
            pltpu.VMEM(staple, f32),
            pltpu.VMEM((12, tiles, LANES), f32),
            pltpu.VMEM((12, tiles, LANES), f32),
            pltpu.VMEM((18, tiles, LANES), f32),
            pltpu.VMEM((18, tiles, LANES), f32),
            pltpu.VMEM((rows, sites), f32),
            pltpu.VMEM(halved, f32),
            pltpu.VMEM(halved, f32),
            pltpu.VMEM(exchanged, f32),
            pltpu.VMEM(exchanged, f32),
            pltpu.VMEM(exchanged, f32),
            pltpu.VMEM(exchanged, f32),
            pltpu.VMEM(halved, f32),
            pltpu.VMEM(halved, f32),
            pltpu.SemaphoreType.DMA((5,)),
            pltpu.SemaphoreType.DMA((8, 2)),
            pltpu.SemaphoreType.DMA((2, 3)),
            pltpu.SemaphoreType.DMA((2, 3)),
            pltpu.SemaphoreType.REGULAR((2 * gx_count.bit_length(),)),
        ],
        compiler_params=pltpu.CompilerParams(collective_id=0, has_side_effects=True, **PARAMS),
        name="momentum_and_smooth",
    )(links, momentum.reshape(field), jnp.asarray(plane), jnp.asarray(modes, f32), x_table, y_squares)

    width = 2 * LANES
    new_link, new_momentum = pl.pallas_call(
        finish_kernel,
        grid=(sites // width,),
        out_shape=[jax.ShapeDtypeStruct(links.shape[1:], f32), jax.ShapeDtypeStruct(field, f32)],
        in_specs=[
            pl.BlockSpec((rows, width), lambda i: (0, i)),
            pl.BlockSpec((1, 12, local_y, width), lambda i: (0, 0, 0, i)),
            pl.BlockSpec((channels, local_y, width), lambda i: (0, 0, i)),
        ],
        out_specs=[
            pl.BlockSpec((12, local_y, width), lambda i: (0, 0, i)),
            pl.BlockSpec((channels, local_y, width), lambda i: (0, 0, i)),
        ],
        compiler_params=pltpu.CompilerParams(**PARAMS),
        name="link_update",
    )(smooth, links, new_momentum)
    return (new_momentum.reshape(momentum.shape), new_link.reshape(12, 1, local_y, sites))


def solution(mesh):
    return jax.shard_map(
        shards,
        mesh=mesh,
        in_specs=(P(None, None, ("cfg", "gx"), "gy", None), P(None, ("cfg", "gx"), "gy", None)),
        out_specs=(P(None, ("cfg", "gx"), "gy", None), P(None, ("cfg", "gx"), "gy", None)),
        check_vma=False,
    )
```

```python
import functools
import math

import jax
import jax.numpy as jnp
import numpy as np
from jax import lax
from jax.experimental import pallas as pl
from jax.experimental.pallas import tpu as pltpu
from jax.sharding import PartitionSpec as P

NZ = 32
NT = 32
LANES = 128

coupling = 6.0
step_force = 0.3
step_link = 0.15
kernel_mass = 0.01

f32 = jnp.float32
bf16 = jnp.bfloat16
VMEM = pl.BlockSpec(memory_space=pltpu.VMEM)
PARAMS = dict(vmem_limit_bytes=60 * 1024 * 1024)


def hartley(length):
    index = np.arange(length)
    angle = 2.0 * np.pi * (np.outer(index, index) % length) / length
    return np.cos(angle) + np.sin(angle)


def in_two(table):
    high = jnp.asarray(table, f32).astype(bf16)
    return high, (jnp.asarray(table, f32) - high.astype(f32)).astype(bf16)


def cdot(lefts, rights, conj_left=False, conj_right=False):
    re = im = None
    for (a, b), (c, d) in zip(lefts, rights):
        same = conj_left == conj_right
        re_term = a * c - b * d if same else a * c + b * d
        if not conj_left and not conj_right:
            im_term = a * d + b * c
        elif conj_left and not conj_right:
            im_term = a * d - b * c
        elif conj_right and not conj_left:
            im_term = b * c - a * d
        else:
            im_term = -(a * d + b * c)
        re = re_term if re is None else re + re_term
        im = im_term if im is None else im + im_term
    return re, im


def product(left, right, adj_left=False, adj_right=False):
    out = []
    for r in range(3):
        row = []
        lefts = [left[k][r] for k in range(3)] if adj_left else [left[r][k] for k in range(3)]
        for c in range(3):
            rights = [right[c][k] for k in range(3)] if adj_right else [right[k][c] for k in range(3)]
            row.append(cdot(lefts, rights, adj_left, adj_right))
        out.append(row)
    return out


def with_third(rows):
    third = []
    for k in range(3):
        i, j = (k + 1) % 3, (k + 2) % 3
        (a, b), (c, d) = rows[0][i], rows[1][j]
        (e, f), (g, h) = rows[0][j], rows[1][i]
        third.append(((a * c - b * d) - (e * g - f * h), (e * h + f * g) - (a * d + b * c)))
    return [rows[0], rows[1], third]


def matrix_of(get):
    return with_third([[(get(3 * r + k), get(6 + 3 * r + k)) for k in range(3)] for r in range(2)])


def algebra_parts(m):
    inv_root = 1.0 / math.sqrt(3.0)
    return [
        m[1][0][1] + m[0][1][1],
        m[0][1][0] - m[1][0][0],
        m[0][0][1] - m[1][1][1],
        m[2][0][1] + m[0][2][1],
        m[0][2][0] - m[2][0][0],
        m[2][1][1] + m[1][2][1],
        m[1][2][0] - m[2][1][0],
        (m[0][0][1] + m[1][1][1] - 2.0 * m[2][2][1]) * inv_root,
    ]


def split_dot(value, high_ref, low_ref, columns, rows=slice(None)):
    high = value.astype(bf16)
    low = (value - high.astype(f32)).astype(bf16)
    table = high_ref[rows, columns]
    return (
        jnp.dot(high, table, preferred_element_type=f32)
        + jnp.dot(low, table, preferred_element_type=f32)
        + jnp.dot(high, low_ref[rows, columns], preferred_element_type=f32)
    )


def finish_kernel(smooth_ref, links_ref, momentum_ref, new_ref, copied_ref):
    copied_ref[...] = momentum_ref[...]
    tiles = new_ref.shape[2] // LANES
    root_inv = 1.0 / math.sqrt(3.0)
    scale = 0.25 * step_link * 0.5

    def one(i, carry):
        here = pl.ds(pl.multiple_of(i * LANES, LANES), LANES)
        s = [smooth_ref[pl.ds(8 * a, 8), here] * scale for a in range(8)]
        eighth = root_inv * s[7]
        h00, h11, h22 = eighth + s[2], eighth - s[2], -2.0 * eighth
        a01, b01 = s[0], -s[1]
        a02, b02 = s[3], -s[4]
        a12, b12 = s[5], -s[6]
        n01 = a01 * a01 + b01 * b01
        n02 = a02 * a02 + b02 * b02
        n12 = a12 * a12 + b12 * b12
        p = 0.5 * (h00 * h00 + h11 * h11 + h22 * h22) + (n01 + n02 + n12)
        m_re = a01 * a12 - b01 * b12
        m_im = a01 * b12 + b01 * a12
        q = h00 * h11 * h22 + 2.0 * (m_re * a02 + m_im * b02) - h00 * n12 - h11 * n02 - h22 * n01
        pq = p * q
        pp = p * p
        c0 = (1.0 - q * q * (1.0 / 720.0), pq * (1.0 / 120.0) - q * (1.0 / 6.0))
        c1 = (q * (1.0 / 24.0) - pq * (1.0 / 360.0), 1.0 - p * (1.0 / 6.0) + pp * (1.0 / 120.0))
        c2 = (p * (1.0 / 24.0) - 0.5 - pp * (1.0 / 720.0), q * (1.0 / 120.0))

        def cm(u, v):
            return (u[0] * v[0] - u[1] * v[1], u[0] * v[1] + u[1] * v[0])

        for _ in range(2):
            s00, s11, s22 = cm(c0, c0), cm(c1, c1), cm(c2, c2)
            d01, d02, d12 = cm(c0, c1), cm(c0, c2), cm(c1, c2)
            c0, c1, c2 = (
                tuple(s00[x] + 2.0 * q * d12[x] for x in range(2)),
                tuple(2.0 * (d01[x] + p * d12[x]) + q * s22[x] for x in range(2)),
                tuple(2.0 * d02[x] + s11[x] + p * s22[x] for x in range(2)),
            )
        g00 = h00 * h00 + n01 + n02
        g11 = h11 * h11 + n01 + n12
        g01 = (a01 * (h00 + h11) + a02 * a12 + b02 * b12, b01 * (h00 + h11) + b02 * a12 - a02 * b12)
        g02 = (a02 * (h00 + h22) + m_re, b02 * (h00 + h22) + m_im)
        g12 = (a12 * (h11 + h22) + a01 * a02 + b01 * b02, b12 * (h11 + h22) + a01 * b02 - b01 * a02)

        def mix(h, g):
            first, second = cm(c1, h), cm(c2, g)
            return (first[0] + second[0], first[1] + second[1])

        def diagonal(h, g):
            return (c0[0] + c1[0] * h + c2[0] * g, c0[1] + c1[1] * h + c2[1] * g)

        rotation = [
            [diagonal(h00, g00), mix((a01, b01), g01), mix((a02, b02), g02)],
            [mix((a01, -b01), (g01[0], -g01[1])), diagonal(h11, g11), mix((a12, b12), g12)],
        ]
        link = matrix_of(lambda e: links_ref[0, e, :, here])
        for r in range(2):
            for k in range(3):
                re, im = cdot(rotation[r], [link[m][k] for m in range(3)])
                new_ref[3 * r + k, :, here] = re
                new_ref[6 + 3 * r + k, :, here] = im
        return carry

    lax.fori_loop(0, tiles, one, 0)


def step_kernel(
    inner, outer, y_table,
    links_hbm, momentum_hbm, plane_hbm, modes_hbm, x_hbm, y_squares,
    new_ref, smooth_ref,
    links_ref, ahead_ref, momentum_ref, plane_ref, modes_ref, x_ref,
    high_ref, low_ref, weight_ref, path_ref, partial_ref, staple_ref, behind_ref,
    top_out, top_in, edge_out, edge_in,
    plane_sum_ref, spectrum_ref, both_ref, bands_ref, whole_ref, done_ref, back_ref, halves_ref, filtered_ref,
    load_sems, halo_sems, swap_sems, all_sems, ring_sems,
):
    me = lax.axis_index("gx")
    core = lax.axis_index("gy")
    other = 1 - core
    peers = inner * outer
    row = me // inner
    col = me % inner
    mesh_id = pl.DeviceIdType.MESH
    part = lax.axis_index("cfg")

    def wrapped(value, count):
        return lax.select(value >= count, value - count, value)

    def at(place):
        return (part, place, core)

    def in_row(step):
        return at(row * inner + wrapped(col + step % inner, inner))

    def in_column(step):
        return at(wrapped(row + step % outer, outer) * inner + col)

    before = at(wrapped(me + peers - 1, peers))
    after = at(wrapped(me + 1, peers))
    partner = (part, me, other)
    col_before, col_after = in_row(-1), in_row(1)
    row_before, row_after = in_column(-1), in_column(1)
    neighbours = (before, after, partner, col_before, col_after, row_before, row_after)

    def signal(sem, device):
        pl.semaphore_signal(sem, inc=1, device_id=device, device_id_type=mesh_id)

    def send(source, target, sems, device):
        return pltpu.make_async_remote_copy(
            src_ref=source, dst_ref=target, send_sem=sems.at[0], recv_sem=sems.at[1],
            device_id=device, device_id_type=mesh_id,
        )

    barrier = pltpu.get_barrier_semaphore()
    for device in neighbours:
        signal(barrier, device)
    loads = [
        pltpu.make_async_copy(links_hbm, links_ref, load_sems.at[0]),
        pltpu.make_async_copy(plane_hbm, plane_ref, load_sems.at[1]),
        pltpu.make_async_copy(modes_hbm.at[core], modes_ref, load_sems.at[2]),
        pltpu.make_async_copy(x_hbm, x_ref, load_sems.at[3]),
        pltpu.make_async_copy(momentum_hbm, momentum_ref, load_sems.at[4]),
    ]
    for load in loads:
        load.start()
    pl.semaphore_wait(barrier, len(neighbours))

    sites = new_ref.shape[2]
    halos = [send(links_hbm.at[nu], ahead_ref.at[nu - 1], halo_sems.at[nu - 1], before) for nu in (1, 2)]
    quarters = 4
    width = sites // quarters
    for q in range(quarters):
        lanes = pl.ds(q * width, width)
        halos.append(
            send(links_hbm.at[3, :, :, lanes], ahead_ref.at[2, :, :, lanes], halo_sems.at[2 + q], before)
        )
    for halo in halos:
        halo.start()

    def relay(steps, behind, ahead, first):
        def step(k, carry):
            signal(ring_sems.at[first], ahead)
            signal(ring_sems.at[first + 1], behind)
            pl.semaphore_wait(ring_sems.at[first], 1)
            pl.semaphore_wait(ring_sems.at[first + 1], 1)
            return carry

        lax.fori_loop(0, steps, step, 0)

    tiles = new_ref.shape[2] // LANES
    lane = lax.broadcasted_iota(jnp.int32, (8, LANES), 1)
    sublane = lax.broadcasted_iota(jnp.int32, (8, LANES), 0)
    t_site = lane % NT

    def lanes_of(i):
        return pl.ds(pl.multiple_of(i * LANES, LANES), LANES)

    loads[0].wait()

    def pack_top(i, carry):
        for e in range(12):
            top_out[e, pl.ds(i, 1), :] = links_ref[0, e, 0:1, lanes_of(i)]
        return carry

    lax.fori_loop(0, tiles, pack_top, 0)
    top = send(top_out, top_in, halo_sems.at[2 + quarters], partner)
    top.start()

    for load in loads[1:]:
        load.wait()

    def table_block(z, carry):
        full = plane_ref[0] * plane_ref[1, pl.ds(z, 1), :]
        high = full.astype(bf16)
        rows = pl.ds(pl.multiple_of(z * NT, NT), NT)
        high_ref[rows, :] = high
        low_ref[rows, :] = (full - high.astype(f32)).astype(bf16)
        return carry

    lax.fori_loop(0, NZ, table_block, 0)
    scale = 4.0 / (peers * inner * NZ * NT)
    weight_ref[...] = scale / (kernel_mass + 4.0 * (modes_ref[...] + y_squares[col]))
    relay(inner // 2, col_before, col_after, 0)
    relay(outer // 2, row_before, row_after, 2)
    top.wait()

    def prepare(i, carry):
        here = lanes_of(i)
        following = lanes_of(lax.rem(i + 1, tiles))

        def moved_y(e):
            edge = jnp.broadcast_to(top_in[e, pl.ds(i, 1), :], (8, LANES))
            return jnp.where(sublane == 7, edge, pltpu.roll(links_ref[0, e, :, here], 7, 0))

        def moved_z(e):
            return jnp.where(
                lane < LANES - NT,
                pltpu.roll(links_ref[0, e, :, here], LANES - NT, 1),
                pltpu.roll(links_ref[0, e, :, following], LANES - NT, 1),
            )

        def moved_t(e):
            value = links_ref[0, e, :, here]
            return jnp.where(
                t_site == NT - 1, pltpu.roll(value, NT - 1, 1), pltpu.roll(value, LANES - 1, 1)
            )

        for nu, moved in ((1, moved_y), (2, moved_z), (3, moved_t)):
            link_nu = matrix_of(lambda e: links_ref[nu, e, :, here])
            path = product(link_nu, matrix_of(moved))
            for r in range(3):
                for k in range(3):
                    path_ref[nu - 1, 3 * r + k, :, here] = path[r][k][0]
                    path_ref[nu - 1, 9 + 3 * r + k, :, here] = path[r][k][1]
        return carry

    lax.fori_loop(0, tiles, prepare, 0)

    def staples(nu, i):
        here = lanes_of(i)
        link_x = matrix_of(lambda e: links_ref[0, e, :, here])
        link_nu = matrix_of(lambda e: links_ref[nu, e, :, here])
        ahead = matrix_of(lambda e: ahead_ref[nu - 1, e, :, here])
        corner = product(link_x, ahead)
        lower = product(corner, link_nu, adj_left=True)
        path = [
            [(path_ref[nu - 1, 3 * r + k, :, here], path_ref[nu - 1, 9 + 3 * r + k, :, here]) for k in range(3)]
            for r in range(3)
        ]
        parts = algebra_parts(product(corner, path, adj_right=True))
        for a in range(8):
            if nu == 1:
                partial_ref[a, :, here] = parts[a]
            else:
                partial_ref[a, :, here] += parts[a]
        return here, [lower[r][k][p] for p in range(2) for r in range(3) for k in range(3)]

    def along_y(i, carry):
        here, flat = staples(1, i)
        for e in range(18):
            edge_out[e, pl.ds(i, 1), :] = flat[e][7:8, :]
            staple_ref[e, :, here] = jnp.where(sublane == 0, 0.0, pltpu.roll(flat[e], 1, 0))
        return carry

    def along_z(i, carry):
        here, flat = staples(2, i)
        for e in range(18):
            behind_ref[e, :, here] = flat[e]
        return carry

    def along_t(i, carry):
        here, flat = staples(3, i)
        for e in range(18):
            staple_ref[e, :, here] += jnp.where(
                t_site == 0, pltpu.roll(flat[e], LANES - NT + 1, 1), pltpu.roll(flat[e], 1, 1)
            )
        return carry

    halos[0].wait_recv()
    lax.fori_loop(0, tiles, along_y, 0)
    edge = send(edge_out, edge_in, halo_sems.at[3 + quarters], partner)
    edge.start()
    halos[1].wait_recv()
    lax.fori_loop(0, tiles, along_z, 0)
    edge.wait()

    def force(i, carry):
        here = lanes_of(i)
        previous = lanes_of(lax.rem(i + tiles - 1, tiles))
        flat = [
            staple_ref[e, :, here]
            + jnp.where(sublane == 0, jnp.broadcast_to(edge_in[e, pl.ds(i, 1), :], (8, LANES)), 0.0)
            + jnp.where(
                lane >= NT,
                pltpu.roll(behind_ref[e, :, here], NT, 1),
                pltpu.roll(behind_ref[e, :, previous], NT, 1),
            )
            for e in range(18)
        ]
        staple = [[(flat[3 * r + k], flat[9 + 3 * r + k]) for k in range(3)] for r in range(3)]
        link_x = matrix_of(lambda e: links_ref[0, e, :, here])
        parts = algebra_parts(product(link_x, staple))
        for a in range(8):
            total = (coupling / 6.0) * (partial_ref[a, :, here] + parts[a])
            new_ref[a, :, here] = momentum_ref[a, :, here] - step_force * total
        return carry

    count = new_ref.shape[0] * new_ref.shape[1]
    half = tiles // 2
    per = tiles // quarters
    for q in range(quarters):
        halos[2 + q].wait_recv()
        lax.fori_loop(per * q, per * (q + 1), along_t, 0)
        lax.fori_loop(per * q, per * (q + 1), force, 0)
        taken = slice(q * width, (q + 1) * width)
        value = new_ref[:, :, taken].reshape(count, width)
        for pair in range(half):
            columns = slice(pair * 2 * LANES, (pair + 1) * 2 * LANES)
            out = split_dot(value, high_ref, low_ref, columns, taken)
            if q:
                out = out + plane_sum_ref[:, columns]
            if q < quarters - 1:
                plane_sum_ref[:, columns] = out
                continue
            for side in range(2):
                tile = 2 * pair + side
                spectrum_ref[tile // half, pl.ds(tile % half, count, stride=half), :] = out[
                    :, side * LANES : (side + 1) * LANES
                ]

    def swap(source, target, stage):
        remote = send(source.at[other], target.at[core], swap_sems.at[stage], partner)
        remote.start()
        local = pltpu.make_async_copy(source.at[core], target.at[core], swap_sems.at[stage, 2])
        local.start()
        local.wait()
        remote.wait()

    def all_to_all(source, target, stage):
        def push(to):
            send(source.at[to], target.at[me], all_sems.at[stage], at(to)).start()

        def begin(d, carry):
            push(wrapped(me + d, peers))
            push(wrapped(me + peers - d, peers))
            return carry

        lax.fori_loop(1, peers // 2, begin, 0)
        push(wrapped(me + peers // 2, peers))
        local = pltpu.make_async_copy(source.at[me], target.at[me], all_sems.at[stage, 2])
        local.start()
        local.wait()
        rest = pl.ds(0, peers - 1)
        pltpu.make_async_copy(source.at[rest], source.at[rest], all_sems.at[stage, 0]).wait()
        pltpu.make_async_copy(target.at[rest], target.at[rest], all_sems.at[stage, 1]).wait()

    swap(spectrum_ref, both_ref, 0)
    local_y = new_ref.shape[1]
    total_y = 2 * local_y

    def lines_of(c, y):
        return pl.ds(pl.multiple_of(c * (local_y * half), local_y * half) + (y % local_y) * half, half)

    def forward_y(c, carry):
        lines = [both_ref[y // local_y, lines_of(c, y), :] for y in range(total_y)]
        for k in range(total_y):
            total = None
            for y in range(total_y):
                term = float(y_table[k, y]) * lines[y]
                total = term if total is None else total + term
            bands_ref[c * inner + k] = total
        return carry

    lax.fori_loop(0, outer, forward_y, 0)
    all_to_all(bands_ref, whole_ref, 0)

    shape = whole_ref.shape
    flat_shape = (shape[0] * shape[1], shape[2])

    def transform(value):
        high = value.astype(bf16)
        low = (value - high.astype(f32)).astype(bf16)
        table = x_ref[0]
        return (
            jnp.dot(table, high, preferred_element_type=f32)
            + jnp.dot(table, low, preferred_element_type=f32)
            + jnp.dot(x_ref[1], high, preferred_element_type=f32)
        )

    modes = transform(whole_ref[...].reshape(flat_shape)) * weight_ref[...]
    done_ref[...] = transform(modes).reshape(shape)
    all_to_all(done_ref, back_ref, 1)

    def inverse_y(c, carry):
        lines = [back_ref[c * inner + k] for k in range(total_y)]
        for y in range(total_y):
            total = None
            for k in range(total_y):
                term = float(y_table[k, y]) * lines[k]
                total = term if total is None else total + term
            halves_ref[y // local_y, lines_of(c, y), :] = total
        return carry

    lax.fori_loop(0, outer, inverse_y, 0)
    swap(halves_ref, filtered_ref, 1)
    value = jnp.concatenate(
        [filtered_ref[tile // half, pl.ds(tile % half, count, stride=half), :] for tile in range(tiles)],
        axis=1,
    )
    for pair in range(half):
        columns = slice(pair * 2 * LANES, (pair + 1) * 2 * LANES)
        smooth_ref[:, columns] = split_dot(value, high_ref, low_ref, columns)
    for halo in halos:
        halo.wait_send()


def sine_squares(length):
    return np.sin(np.pi * np.arange(length) / length) ** 2


def shards(gauge_links, momentum):
    channels, _, local_y, sites = momentum.shape
    gx_count = lax.axis_size("gx")
    inner = 2 * local_y
    outer = channels
    tiles = sites // LANES
    half = tiles // 2
    rows = channels * local_y
    links = gauge_links.reshape(4, 12, local_y, sites)
    field = (channels, local_y, sites)

    plane = np.stack([np.tile(hartley(NT), (1, NZ)), np.repeat(hartley(NZ), NT, axis=1)]).astype(np.float32)
    index = np.arange(sites)
    z_t = (sine_squares(NZ)[index // NT] + sine_squares(NT)[index % NT]).reshape(2, half, LANES)
    modes = np.tile(z_t, (1, gx_count, 1)) + np.repeat(sine_squares(gx_count), half)[None, :, None]
    x_high, x_low = in_two(np.kron(hartley(gx_count), np.eye(half)).astype(np.float32))
    x_table = jnp.stack([x_high, x_low])
    y_squares = jnp.asarray(sine_squares(inner), f32)

    any_spec = pl.BlockSpec(memory_space=pl.ANY)
    exchanged = (gx_count, half, LANES)
    halved = (2, rows * half, LANES)
    staple = (18, local_y, sites)
    new_momentum, smooth = pl.pallas_call(
        functools.partial(step_kernel, inner, outer, hartley(inner)),
        out_shape=[jax.ShapeDtypeStruct(field, f32), jax.ShapeDtypeStruct((rows, sites), f32)],
        in_specs=[any_spec] * 5 + [pl.BlockSpec(memory_space=pltpu.SMEM)],
        out_specs=[VMEM] * 2,
        scratch_shapes=[
            pltpu.VMEM(links.shape, f32),
            pltpu.VMEM((3,) + links.shape[1:], f32),
            pltpu.VMEM(field, f32),
            pltpu.VMEM(plane.shape, f32),
            pltpu.VMEM(modes.shape[1:], f32),
            pltpu.VMEM(x_table.shape, bf16),
            pltpu.VMEM((sites, sites), bf16),
            pltpu.VMEM((sites, sites), bf16),
            pltpu.VMEM(modes.shape[1:], f32),
            pltpu.VMEM((3,) + staple, f32),
            pltpu.VMEM(field, f32),
            pltpu.VMEM(staple, f32),
            pltpu.VMEM(staple, f32),
            pltpu.VMEM((12, tiles, LANES), f32),
            pltpu.VMEM((12, tiles, LANES), f32),
            pltpu.VMEM((18, tiles, LANES), f32),
            pltpu.VMEM((18, tiles, LANES), f32),
            pltpu.VMEM((rows, sites), f32),
            pltpu.VMEM(halved, f32),
            pltpu.VMEM(halved, f32),
            pltpu.VMEM(exchanged, f32),
            pltpu.VMEM(exchanged, f32),
            pltpu.VMEM(exchanged, f32),
            pltpu.VMEM(exchanged, f32),
            pltpu.VMEM(halved, f32),
            pltpu.VMEM(halved, f32),
            pltpu.SemaphoreType.DMA((5,)),
            pltpu.SemaphoreType.DMA((8, 2)),
            pltpu.SemaphoreType.DMA((2, 3)),
            pltpu.SemaphoreType.DMA((2, 3)),
            pltpu.SemaphoreType.REGULAR((4,)),
        ],
        compiler_params=pltpu.CompilerParams(collective_id=0, has_side_effects=True, **PARAMS),
        name="momentum_and_smooth",
    )(links, momentum.reshape(field), jnp.asarray(plane), jnp.asarray(modes, f32), x_table, y_squares)

    width = 2 * LANES
    new_link, new_momentum = pl.pallas_call(
        finish_kernel,
        grid=(sites // width,),
        out_shape=[jax.ShapeDtypeStruct(links.shape[1:], f32), jax.ShapeDtypeStruct(field, f32)],
        in_specs=[
            pl.BlockSpec((rows, width), lambda i: (0, i)),
            pl.BlockSpec((1, 12, local_y, width), lambda i: (0, 0, 0, i)),
            pl.BlockSpec((channels, local_y, width), lambda i: (0, 0, i)),
        ],
        out_specs=[
            pl.BlockSpec((12, local_y, width), lambda i: (0, 0, i)),
            pl.BlockSpec((channels, local_y, width), lambda i: (0, 0, i)),
        ],
        compiler_params=pltpu.CompilerParams(**PARAMS),
        name="link_update",
    )(smooth, links, new_momentum)
    return (new_momentum.reshape(momentum.shape), new_link.reshape(12, 1, local_y, sites))


def solution(mesh):
    return jax.shard_map(
        shards,
        mesh=mesh,
        in_specs=(P(None, None, ("cfg", "gx"), "gy", None), P(None, ("cfg", "gx"), "gy", None)),
        out_specs=(P(None, ("cfg", "gx"), "gy", None), P(None, ("cfg", "gx"), "gy", None)),
        check_vma=False,
    )
```

```python
import functools
import math

import jax
import jax.numpy as jnp
import numpy as np
from jax import lax
from jax.experimental import pallas as pl
from jax.experimental.pallas import tpu as pltpu
from jax.sharding import PartitionSpec as P

NZ = 32
NT = 32
LANES = 128

coupling = 6.0
step_force = 0.3
step_link = 0.15
kernel_mass = 0.01

f32 = jnp.float32
bf16 = jnp.bfloat16
VMEM = pl.BlockSpec(memory_space=pltpu.VMEM)
PARAMS = dict(vmem_limit_bytes=60 * 1024 * 1024)


def hartley(length):
    index = np.arange(length)
    angle = 2.0 * np.pi * (np.outer(index, index) % length) / length
    return np.cos(angle) + np.sin(angle)


def in_two(table):
    high = jnp.asarray(table, f32).astype(bf16)
    return high, (jnp.asarray(table, f32) - high.astype(f32)).astype(bf16)


def cdot(lefts, rights, conj_left=False, conj_right=False):
    re = im = None
    for (a, b), (c, d) in zip(lefts, rights):
        same = conj_left == conj_right
        re_term = a * c - b * d if same else a * c + b * d
        if not conj_left and not conj_right:
            im_term = a * d + b * c
        elif conj_left and not conj_right:
            im_term = a * d - b * c
        elif conj_right and not conj_left:
            im_term = b * c - a * d
        else:
            im_term = -(a * d + b * c)
        re = re_term if re is None else re + re_term
        im = im_term if im is None else im + im_term
    return re, im


def product(left, right, adj_left=False, adj_right=False):
    out = []
    for r in range(3):
        row = []
        lefts = [left[k][r] for k in range(3)] if adj_left else [left[r][k] for k in range(3)]
        for c in range(3):
            rights = [right[c][k] for k in range(3)] if adj_right else [right[k][c] for k in range(3)]
            row.append(cdot(lefts, rights, adj_left, adj_right))
        out.append(row)
    return out


def with_third(rows):
    third = []
    for k in range(3):
        i, j = (k + 1) % 3, (k + 2) % 3
        (a, b), (c, d) = rows[0][i], rows[1][j]
        (e, f), (g, h) = rows[0][j], rows[1][i]
        third.append(((a * c - b * d) - (e * g - f * h), (e * h + f * g) - (a * d + b * c)))
    return [rows[0], rows[1], third]


def matrix_of(get):
    return with_third([[(get(3 * r + k), get(6 + 3 * r + k)) for k in range(3)] for r in range(2)])


def algebra_parts(m):
    inv_root = 1.0 / math.sqrt(3.0)
    return [
        m[1][0][1] + m[0][1][1],
        m[0][1][0] - m[1][0][0],
        m[0][0][1] - m[1][1][1],
        m[2][0][1] + m[0][2][1],
        m[0][2][0] - m[2][0][0],
        m[2][1][1] + m[1][2][1],
        m[1][2][0] - m[2][1][0],
        (m[0][0][1] + m[1][1][1] - 2.0 * m[2][2][1]) * inv_root,
    ]


def split_dot(value, high_ref, low_ref, columns, rows=slice(None)):
    high = value.astype(bf16)
    low = (value - high.astype(f32)).astype(bf16)
    table = high_ref[rows, columns]
    return (
        jnp.dot(high, table, preferred_element_type=f32)
        + jnp.dot(low, table, preferred_element_type=f32)
        + jnp.dot(high, low_ref[rows, columns], preferred_element_type=f32)
    )


def finish_kernel(smooth_ref, links_ref, momentum_ref, new_ref, copied_ref):
    copied_ref[...] = momentum_ref[...]
    tiles = new_ref.shape[2] // LANES
    root_inv = 1.0 / math.sqrt(3.0)
    scale = 0.25 * step_link * 0.5

    def one(i, carry):
        here = pl.ds(pl.multiple_of(i * LANES, LANES), LANES)
        s = [smooth_ref[pl.ds(8 * a, 8), here] * scale for a in range(8)]
        eighth = root_inv * s[7]
        h00, h11, h22 = eighth + s[2], eighth - s[2], -2.0 * eighth
        a01, b01 = s[0], -s[1]
        a02, b02 = s[3], -s[4]
        a12, b12 = s[5], -s[6]
        n01 = a01 * a01 + b01 * b01
        n02 = a02 * a02 + b02 * b02
        n12 = a12 * a12 + b12 * b12
        p = 0.5 * (h00 * h00 + h11 * h11 + h22 * h22) + (n01 + n02 + n12)
        m_re = a01 * a12 - b01 * b12
        m_im = a01 * b12 + b01 * a12
        q = h00 * h11 * h22 + 2.0 * (m_re * a02 + m_im * b02) - h00 * n12 - h11 * n02 - h22 * n01
        pq = p * q
        pp = p * p
        c0 = (1.0 - q * q * (1.0 / 720.0), pq * (1.0 / 120.0) - q * (1.0 / 6.0))
        c1 = (q * (1.0 / 24.0) - pq * (1.0 / 360.0), 1.0 - p * (1.0 / 6.0) + pp * (1.0 / 120.0))
        c2 = (p * (1.0 / 24.0) - 0.5 - pp * (1.0 / 720.0), q * (1.0 / 120.0))

        def cm(u, v):
            return (u[0] * v[0] - u[1] * v[1], u[0] * v[1] + u[1] * v[0])

        for _ in range(2):
            s00, s11, s22 = cm(c0, c0), cm(c1, c1), cm(c2, c2)
            d01, d02, d12 = cm(c0, c1), cm(c0, c2), cm(c1, c2)
            c0, c1, c2 = (
                tuple(s00[x] + 2.0 * q * d12[x] for x in range(2)),
                tuple(2.0 * (d01[x] + p * d12[x]) + q * s22[x] for x in range(2)),
                tuple(2.0 * d02[x] + s11[x] + p * s22[x] for x in range(2)),
            )
        g00 = h00 * h00 + n01 + n02
        g11 = h11 * h11 + n01 + n12
        g01 = (a01 * (h00 + h11) + a02 * a12 + b02 * b12, b01 * (h00 + h11) + b02 * a12 - a02 * b12)
        g02 = (a02 * (h00 + h22) + m_re, b02 * (h00 + h22) + m_im)
        g12 = (a12 * (h11 + h22) + a01 * a02 + b01 * b02, b12 * (h11 + h22) + a01 * b02 - b01 * a02)

        def mix(h, g):
            first, second = cm(c1, h), cm(c2, g)
            return (first[0] + second[0], first[1] + second[1])

        def diagonal(h, g):
            return (c0[0] + c1[0] * h + c2[0] * g, c0[1] + c1[1] * h + c2[1] * g)

        rotation = [
            [diagonal(h00, g00), mix((a01, b01), g01), mix((a02, b02), g02)],
            [mix((a01, -b01), (g01[0], -g01[1])), diagonal(h11, g11), mix((a12, b12), g12)],
        ]
        link = matrix_of(lambda e: links_ref[0, e, :, here])
        for r in range(2):
            for k in range(3):
                re, im = cdot(rotation[r], [link[m][k] for m in range(3)])
                new_ref[3 * r + k, :, here] = re
                new_ref[6 + 3 * r + k, :, here] = im
        return carry

    lax.fori_loop(0, tiles, one, 0)


def step_kernel(
    inner, outer, y_table,
    links_hbm, momentum_hbm, plane_hbm, modes_hbm, x_hbm, y_squares,
    new_ref, smooth_ref,
    links_ref, ahead_ref, momentum_ref, plane_ref, modes_ref, x_ref,
    high_ref, low_ref, weight_ref, path_ref, partial_ref, staple_ref, behind_ref,
    turn_x, turn_t, parts_out, parts_in, top_out, top_in, edge_out, edge_in,
    plane_sum_ref, spectrum_ref, both_ref, bands_ref, whole_ref, done_ref, back_ref, halves_ref, filtered_ref,
    load_sems, halo_sems, swap_sems, all_sems, ring_sems,
):
    me = lax.axis_index("gx")
    core = lax.axis_index("gy")
    other = 1 - core
    peers = inner * outer
    row = me // inner
    col = me % inner
    mesh_id = pl.DeviceIdType.MESH
    part = lax.axis_index("cfg")

    def wrapped(value, count):
        return lax.select(value >= count, value - count, value)

    def at(place):
        return (part, place, core)

    def in_row(step):
        return at(row * inner + wrapped(col + step % inner, inner))

    def in_column(step):
        return at(wrapped(row + step % outer, outer) * inner + col)

    before = at(wrapped(me + peers - 1, peers))
    after = at(wrapped(me + 1, peers))
    partner = (part, me, other)
    col_before, col_after = in_row(-1), in_row(1)
    row_before, row_after = in_column(-1), in_column(1)
    neighbours = (before, after, partner, col_before, col_after, row_before, row_after)

    def signal(sem, device):
        pl.semaphore_signal(sem, inc=1, device_id=device, device_id_type=mesh_id)

    def send(source, target, sems, device):
        return pltpu.make_async_remote_copy(
            src_ref=source, dst_ref=target, send_sem=sems.at[0], recv_sem=sems.at[1],
            device_id=device, device_id_type=mesh_id,
        )

    barrier = pltpu.get_barrier_semaphore()
    for device in neighbours:
        signal(barrier, device)
    loads = [
        pltpu.make_async_copy(links_hbm, links_ref, load_sems.at[0]),
        pltpu.make_async_copy(plane_hbm, plane_ref, load_sems.at[1]),
        pltpu.make_async_copy(modes_hbm.at[core], modes_ref, load_sems.at[2]),
        pltpu.make_async_copy(x_hbm, x_ref, load_sems.at[3]),
        pltpu.make_async_copy(momentum_hbm, momentum_ref, load_sems.at[4]),
    ]
    for load in loads:
        load.start()
    pl.semaphore_wait(barrier, len(neighbours))

    sites = new_ref.shape[2]
    halos = [send(links_hbm.at[nu], ahead_ref.at[nu - 1], halo_sems.at[nu - 1], before) for nu in (1, 2)]
    quarters = 4
    width = sites // quarters
    quarter = [pl.ds(q * width, width) for q in range(quarters)]
    halos.append(send(links_hbm.at[0], turn_x, halo_sems.at[2], after))
    for q in range(quarters):
        halos.append(
            send(links_hbm.at[3, :, :, quarter[q]], turn_t.at[:, :, quarter[q]], halo_sems.at[3 + q], after)
        )
    for halo in halos:
        halo.start()

    def relay(count, known, place, stage):
        while known < count // 2:
            distance = max(known, 1)
            signal(ring_sems.at[stage], place(distance))
            signal(ring_sems.at[stage], place(-distance))
            pl.semaphore_wait(ring_sems.at[stage], 2)
            known += distance
            stage += 1
        return stage

    tiles = new_ref.shape[2] // LANES
    lane = lax.broadcasted_iota(jnp.int32, (8, LANES), 1)
    sublane = lax.broadcasted_iota(jnp.int32, (8, LANES), 0)
    t_site = lane % NT

    def lanes_of(i):
        return pl.ds(pl.multiple_of(i * LANES, LANES), LANES)

    loads[0].wait()

    def pack_top(i, carry):
        for e in range(12):
            top_out[e, pl.ds(i, 1), :] = links_ref[0, e, 0:1, lanes_of(i)]
        return carry

    lax.fori_loop(0, tiles, pack_top, 0)
    top = send(top_out, top_in, halo_sems.at[3 + quarters], partner)
    top.start()

    for load in loads[1:]:
        load.wait()

    def table_block(z, carry):
        full = plane_ref[0] * plane_ref[1, pl.ds(z, 1), :]
        high = full.astype(bf16)
        rows = pl.ds(pl.multiple_of(z * NT, NT), NT)
        high_ref[rows, :] = high
        low_ref[rows, :] = (full - high.astype(f32)).astype(bf16)
        return carry

    lax.fori_loop(0, NZ, table_block, 0)
    scale = 4.0 / (peers * inner * NZ * NT)
    weight_ref[...] = scale / (kernel_mass + 4.0 * (modes_ref[...] + y_squares[col]))
    last = relay(inner, 1, in_row, 0)
    top.wait()

    def prepare(i, carry):
        here = lanes_of(i)
        following = lanes_of(lax.rem(i + 1, tiles))

        def moved_y(e):
            edge = jnp.broadcast_to(top_in[e, pl.ds(i, 1), :], (8, LANES))
            return jnp.where(sublane == 7, edge, pltpu.roll(links_ref[0, e, :, here], 7, 0))

        def moved_z(e):
            return jnp.where(
                lane < LANES - NT,
                pltpu.roll(links_ref[0, e, :, here], LANES - NT, 1),
                pltpu.roll(links_ref[0, e, :, following], LANES - NT, 1),
            )

        for nu, moved in ((1, moved_y), (2, moved_z)):
            link_nu = matrix_of(lambda e: links_ref[nu, e, :, here])
            path = product(link_nu, matrix_of(moved))
            for r in range(3):
                for k in range(3):
                    path_ref[nu - 1, 3 * r + k, :, here] = path[r][k][0]
                    path_ref[nu - 1, 9 + 3 * r + k, :, here] = path[r][k][1]
        return carry

    lax.fori_loop(0, tiles, prepare, 0)

    def staples(nu, i):
        here = lanes_of(i)
        link_x = matrix_of(lambda e: links_ref[0, e, :, here])
        link_nu = matrix_of(lambda e: links_ref[nu, e, :, here])
        ahead = matrix_of(lambda e: ahead_ref[nu - 1, e, :, here])
        corner = product(link_x, ahead)
        lower = product(corner, link_nu, adj_left=True)
        path = [
            [(path_ref[nu - 1, 3 * r + k, :, here], path_ref[nu - 1, 9 + 3 * r + k, :, here]) for k in range(3)]
            for r in range(3)
        ]
        parts = algebra_parts(product(corner, path, adj_right=True))
        for a in range(8):
            if nu == 1:
                partial_ref[a, :, here] = parts[a]
            else:
                partial_ref[a, :, here] += parts[a]
        return here, [lower[r][k][p] for p in range(2) for r in range(3) for k in range(3)]

    def along_y(i, carry):
        here, flat = staples(1, i)
        for e in range(18):
            edge_out[e, pl.ds(i, 1), :] = flat[e][7:8, :]
            staple_ref[e, :, here] = jnp.where(sublane == 0, 0.0, pltpu.roll(flat[e], 1, 0))
        return carry

    def along_z(i, carry):
        here, flat = staples(2, i)
        for e in range(18):
            behind_ref[e, :, here] = flat[e]
        return carry

    def shift_t(value, forward):
        if forward:
            return jnp.where(
                t_site == NT - 1, pltpu.roll(value, NT - 1, 1), pltpu.roll(value, LANES - 1, 1)
            )
        return jnp.where(t_site == 0, pltpu.roll(value, LANES - NT + 1, 1), pltpu.roll(value, 1, 1))

    def along_t(i, carry):
        here = lanes_of(i)
        link_x = matrix_of(lambda e: turn_x[e, :, here])
        moved = matrix_of(lambda e: shift_t(turn_x[e, :, here], True))
        link_t = matrix_of(lambda e: turn_t[e, :, here])
        ahead = matrix_of(lambda e: links_ref[3, e, :, here])
        corner = product(link_x, ahead)
        lower = product(corner, link_t, adj_left=True)
        lower = [[tuple(shift_t(v, False) for v in entry) for entry in line] for line in lower]
        upper = algebra_parts(product(corner, product(link_t, moved), adj_right=True))
        below = algebra_parts(product(link_x, lower))
        for a in range(8):
            parts_out[a, :, here] = upper[a] + below[a]
        return carry

    halos[0].wait_recv()
    lax.fori_loop(0, tiles, along_y, 0)
    edge = send(edge_out, edge_in, halo_sems.at[4 + quarters], partner)
    edge.start()
    relay(outer, 0, in_column, last)
    per = tiles // quarters
    returned = []
    halos[2].wait_recv()
    for q in range(quarters):
        halos[3 + q].wait_recv()
        lax.fori_loop(per * q, per * (q + 1), along_t, 0)
        back = send(
            parts_out.at[:, :, quarter[q]], parts_in.at[:, :, quarter[q]],
            halo_sems.at[5 + quarters + q], before,
        )
        back.start()
        returned.append(back)
    halos[1].wait_recv()
    lax.fori_loop(0, tiles, along_z, 0)
    edge.wait()

    def force(i, carry):
        here = lanes_of(i)
        previous = lanes_of(lax.rem(i + tiles - 1, tiles))
        flat = [
            staple_ref[e, :, here]
            + jnp.where(sublane == 0, jnp.broadcast_to(edge_in[e, pl.ds(i, 1), :], (8, LANES)), 0.0)
            + jnp.where(
                lane >= NT,
                pltpu.roll(behind_ref[e, :, here], NT, 1),
                pltpu.roll(behind_ref[e, :, previous], NT, 1),
            )
            for e in range(18)
        ]
        staple = [[(flat[3 * r + k], flat[9 + 3 * r + k]) for k in range(3)] for r in range(3)]
        link_x = matrix_of(lambda e: links_ref[0, e, :, here])
        parts = algebra_parts(product(link_x, staple))
        for a in range(8):
            total = (coupling / 6.0) * (partial_ref[a, :, here] + parts[a] + parts_in[a, :, here])
            new_ref[a, :, here] = momentum_ref[a, :, here] - step_force * total
        return carry

    count = new_ref.shape[0] * new_ref.shape[1]
    half = tiles // 2
    for q in range(quarters):
        returned[q].wait_recv()
        lax.fori_loop(per * q, per * (q + 1), force, 0)
        taken = slice(q * width, (q + 1) * width)
        value = new_ref[:, :, taken].reshape(count, width)
        for pair in range(half):
            columns = slice(pair * 2 * LANES, (pair + 1) * 2 * LANES)
            out = split_dot(value, high_ref, low_ref, columns, taken)
            if q:
                out = out + plane_sum_ref[:, columns]
            if q < quarters - 1:
                plane_sum_ref[:, columns] = out
                continue
            for side in range(2):
                tile = 2 * pair + side
                spectrum_ref[tile // half, pl.ds(tile % half, count, stride=half), :] = out[
                    :, side * LANES : (side + 1) * LANES
                ]

    def swap(source, target, stage):
        remote = send(source.at[other], target.at[core], swap_sems.at[stage], partner)
        remote.start()
        local = pltpu.make_async_copy(source.at[core], target.at[core], swap_sems.at[stage, 2])
        local.start()
        local.wait()
        remote.wait()

    def all_to_all(source, target, stage):
        def push(to):
            send(source.at[to], target.at[me], all_sems.at[stage], at(to)).start()

        def begin(d, carry):
            push(wrapped(me + d, peers))
            push(wrapped(me + peers - d, peers))
            return carry

        lax.fori_loop(1, peers // 2, begin, 0)
        push(wrapped(me + peers // 2, peers))
        local = pltpu.make_async_copy(source.at[me], target.at[me], all_sems.at[stage, 2])
        local.start()
        local.wait()
        rest = pl.ds(0, peers - 1)
        pltpu.make_async_copy(source.at[rest], source.at[rest], all_sems.at[stage, 0]).wait()
        pltpu.make_async_copy(target.at[rest], target.at[rest], all_sems.at[stage, 1]).wait()

    swap(spectrum_ref, both_ref, 0)
    local_y = new_ref.shape[1]
    total_y = 2 * local_y

    def lines_of(c, y):
        return pl.ds(pl.multiple_of(c * (local_y * half), local_y * half) + (y % local_y) * half, half)

    def forward_y(c, carry):
        lines = [both_ref[y // local_y, lines_of(c, y), :] for y in range(total_y)]
        for k in range(total_y):
            total = None
            for y in range(total_y):
                term = float(y_table[k, y]) * lines[y]
                total = term if total is None else total + term
            bands_ref[c * inner + k] = total
        return carry

    lax.fori_loop(0, outer, forward_y, 0)
    all_to_all(bands_ref, whole_ref, 0)

    shape = whole_ref.shape
    flat_shape = (shape[0] * shape[1], shape[2])

    def transform(value):
        high = value.astype(bf16)
        low = (value - high.astype(f32)).astype(bf16)
        table = x_ref[0]
        return (
            jnp.dot(table, high, preferred_element_type=f32)
            + jnp.dot(table, low, preferred_element_type=f32)
            + jnp.dot(x_ref[1], high, preferred_element_type=f32)
        )

    modes = transform(whole_ref[...].reshape(flat_shape)) * weight_ref[...]
    done_ref[...] = transform(modes).reshape(shape)
    all_to_all(done_ref, back_ref, 1)

    def inverse_y(c, carry):
        lines = [back_ref[c * inner + k] for k in range(total_y)]
        for y in range(total_y):
            total = None
            for k in range(total_y):
                term = float(y_table[k, y]) * lines[k]
                total = term if total is None else total + term
            halves_ref[y // local_y, lines_of(c, y), :] = total
        return carry

    lax.fori_loop(0, outer, inverse_y, 0)
    swap(halves_ref, filtered_ref, 1)
    value = jnp.concatenate(
        [filtered_ref[tile // half, pl.ds(tile % half, count, stride=half), :] for tile in range(tiles)],
        axis=1,
    )
    for pair in range(half):
        columns = slice(pair * 2 * LANES, (pair + 1) * 2 * LANES)
        smooth_ref[:, columns] = split_dot(value, high_ref, low_ref, columns)
    for halo in halos + returned:
        halo.wait_send()


def sine_squares(length):
    return np.sin(np.pi * np.arange(length) / length) ** 2


def shards(gauge_links, momentum):
    channels, _, local_y, sites = momentum.shape
    gx_count = lax.axis_size("gx")
    inner = 2 * local_y
    outer = channels
    tiles = sites // LANES
    half = tiles // 2
    rows = channels * local_y
    links = gauge_links.reshape(4, 12, local_y, sites)
    field = (channels, local_y, sites)

    plane = np.stack([np.tile(hartley(NT), (1, NZ)), np.repeat(hartley(NZ), NT, axis=1)]).astype(np.float32)
    index = np.arange(sites)
    z_t = (sine_squares(NZ)[index // NT] + sine_squares(NT)[index % NT]).reshape(2, half, LANES)
    modes = np.tile(z_t, (1, gx_count, 1)) + np.repeat(sine_squares(gx_count), half)[None, :, None]
    x_high, x_low = in_two(np.kron(hartley(gx_count), np.eye(half)).astype(np.float32))
    x_table = jnp.stack([x_high, x_low])
    y_squares = jnp.asarray(sine_squares(inner), f32)

    any_spec = pl.BlockSpec(memory_space=pl.ANY)
    exchanged = (gx_count, half, LANES)
    halved = (2, rows * half, LANES)
    staple = (18, local_y, sites)
    new_momentum, smooth = pl.pallas_call(
        functools.partial(step_kernel, inner, outer, hartley(inner)),
        out_shape=[jax.ShapeDtypeStruct(field, f32), jax.ShapeDtypeStruct((rows, sites), f32)],
        in_specs=[any_spec] * 5 + [pl.BlockSpec(memory_space=pltpu.SMEM)],
        out_specs=[VMEM] * 2,
        scratch_shapes=[
            pltpu.VMEM(links.shape, f32),
            pltpu.VMEM((2,) + links.shape[1:], f32),
            pltpu.VMEM(field, f32),
            pltpu.VMEM(plane.shape, f32),
            pltpu.VMEM(modes.shape[1:], f32),
            pltpu.VMEM(x_table.shape, bf16),
            pltpu.VMEM((sites, sites), bf16),
            pltpu.VMEM((sites, sites), bf16),
            pltpu.VMEM(modes.shape[1:], f32),
            pltpu.VMEM((2,) + staple, f32),
            pltpu.VMEM(field, f32),
            pltpu.VMEM(staple, f32),
            pltpu.VMEM(staple, f32),
            pltpu.VMEM(links.shape[1:], f32),
            pltpu.VMEM(links.shape[1:], f32),
            pltpu.VMEM(field, f32),
            pltpu.VMEM(field, f32),
            pltpu.VMEM((12, tiles, LANES), f32),
            pltpu.VMEM((12, tiles, LANES), f32),
            pltpu.VMEM((18, tiles, LANES), f32),
            pltpu.VMEM((18, tiles, LANES), f32),
            pltpu.VMEM((rows, sites), f32),
            pltpu.VMEM(halved, f32),
            pltpu.VMEM(halved, f32),
            pltpu.VMEM(exchanged, f32),
            pltpu.VMEM(exchanged, f32),
            pltpu.VMEM(exchanged, f32),
            pltpu.VMEM(exchanged, f32),
            pltpu.VMEM(halved, f32),
            pltpu.VMEM(halved, f32),
            pltpu.SemaphoreType.DMA((5,)),
            pltpu.SemaphoreType.DMA((13, 2)),
            pltpu.SemaphoreType.DMA((2, 3)),
            pltpu.SemaphoreType.DMA((2, 3)),
            pltpu.SemaphoreType.REGULAR((2 * gx_count.bit_length(),)),
        ],
        compiler_params=pltpu.CompilerParams(collective_id=0, has_side_effects=True, **PARAMS),
        name="momentum_and_smooth",
    )(links, momentum.reshape(field), jnp.asarray(plane), jnp.asarray(modes, f32), x_table, y_squares)

    width = 2 * LANES
    new_link, new_momentum = pl.pallas_call(
        finish_kernel,
        grid=(sites // width,),
        out_shape=[jax.ShapeDtypeStruct(links.shape[1:], f32), jax.ShapeDtypeStruct(field, f32)],
        in_specs=[
            pl.BlockSpec((rows, width), lambda i: (0, i)),
            pl.BlockSpec((1, 12, local_y, width), lambda i: (0, 0, 0, i)),
            pl.BlockSpec((channels, local_y, width), lambda i: (0, 0, i)),
        ],
        out_specs=[
            pl.BlockSpec((12, local_y, width), lambda i: (0, 0, i)),
            pl.BlockSpec((channels, local_y, width), lambda i: (0, 0, i)),
        ],
        compiler_params=pltpu.CompilerParams(**PARAMS),
        name="link_update",
    )(smooth, links, new_momentum)
    return (new_momentum.reshape(momentum.shape), new_link.reshape(12, 1, local_y, sites))


def solution(mesh):
    return jax.shard_map(
        shards,
        mesh=mesh,
        in_specs=(P(None, None, ("cfg", "gx"), "gy", None), P(None, ("cfg", "gx"), "gy", None)),
        out_specs=(P(None, ("cfg", "gx"), "gy", None), P(None, ("cfg", "gx"), "gy", None)),
        check_vma=False,
    )
```

```python
import functools
import math

import jax
import jax.numpy as jnp
import numpy as np
from jax import lax
from jax.experimental import pallas as pl
from jax.experimental.pallas import tpu as pltpu
from jax.sharding import PartitionSpec as P

NZ = 32
NT = 32
LANES = 128

coupling = 6.0
step_force = 0.3
step_link = 0.15
kernel_mass = 0.01

f32 = jnp.float32
bf16 = jnp.bfloat16
VMEM = pl.BlockSpec(memory_space=pltpu.VMEM)
PARAMS = dict(vmem_limit_bytes=60 * 1024 * 1024)


def hartley(length):
    index = np.arange(length)
    angle = 2.0 * np.pi * (np.outer(index, index) % length) / length
    return np.cos(angle) + np.sin(angle)


def in_two(table):
    high = jnp.asarray(table, f32).astype(bf16)
    return high, (jnp.asarray(table, f32) - high.astype(f32)).astype(bf16)


def cdot(lefts, rights, conj_left=False, conj_right=False):
    re = im = None
    for (a, b), (c, d) in zip(lefts, rights):
        same = conj_left == conj_right
        re_term = a * c - b * d if same else a * c + b * d
        if not conj_left and not conj_right:
            im_term = a * d + b * c
        elif conj_left and not conj_right:
            im_term = a * d - b * c
        elif conj_right and not conj_left:
            im_term = b * c - a * d
        else:
            im_term = -(a * d + b * c)
        re = re_term if re is None else re + re_term
        im = im_term if im is None else im + im_term
    return re, im


def product(left, right, adj_left=False, adj_right=False):
    out = []
    for r in range(3):
        row = []
        lefts = [left[k][r] for k in range(3)] if adj_left else [left[r][k] for k in range(3)]
        for c in range(3):
            rights = [right[c][k] for k in range(3)] if adj_right else [right[k][c] for k in range(3)]
            row.append(cdot(lefts, rights, adj_left, adj_right))
        out.append(row)
    return out


def with_third(rows):
    third = []
    for k in range(3):
        i, j = (k + 1) % 3, (k + 2) % 3
        (a, b), (c, d) = rows[0][i], rows[1][j]
        (e, f), (g, h) = rows[0][j], rows[1][i]
        third.append(((a * c - b * d) - (e * g - f * h), (e * h + f * g) - (a * d + b * c)))
    return [rows[0], rows[1], third]


def matrix_of(get):
    return with_third([[(get(3 * r + k), get(6 + 3 * r + k)) for k in range(3)] for r in range(2)])


def algebra_parts(m):
    inv_root = 1.0 / math.sqrt(3.0)
    return [
        m[1][0][1] + m[0][1][1],
        m[0][1][0] - m[1][0][0],
        m[0][0][1] - m[1][1][1],
        m[2][0][1] + m[0][2][1],
        m[0][2][0] - m[2][0][0],
        m[2][1][1] + m[1][2][1],
        m[1][2][0] - m[2][1][0],
        (m[0][0][1] + m[1][1][1] - 2.0 * m[2][2][1]) * inv_root,
    ]


def split_dot(value, high_ref, low_ref, columns, rows=slice(None)):
    high = value.astype(bf16)
    low = (value - high.astype(f32)).astype(bf16)
    table = high_ref[rows, columns]
    return (
        jnp.dot(high, table, preferred_element_type=f32)
        + jnp.dot(low, table, preferred_element_type=f32)
        + jnp.dot(high, low_ref[rows, columns], preferred_element_type=f32)
    )


def finish_kernel(smooth_ref, links_ref, momentum_ref, new_ref, copied_ref):
    copied_ref[...] = momentum_ref[...]
    tiles = new_ref.shape[2] // LANES
    root_inv = 1.0 / math.sqrt(3.0)
    scale = 0.25 * step_link * 0.5

    def one(i, carry):
        here = pl.ds(pl.multiple_of(i * LANES, LANES), LANES)
        s = [smooth_ref[pl.ds(8 * a, 8), here] * scale for a in range(8)]
        eighth = root_inv * s[7]
        h00, h11, h22 = eighth + s[2], eighth - s[2], -2.0 * eighth
        a01, b01 = s[0], -s[1]
        a02, b02 = s[3], -s[4]
        a12, b12 = s[5], -s[6]
        n01 = a01 * a01 + b01 * b01
        n02 = a02 * a02 + b02 * b02
        n12 = a12 * a12 + b12 * b12
        p = 0.5 * (h00 * h00 + h11 * h11 + h22 * h22) + (n01 + n02 + n12)
        m_re = a01 * a12 - b01 * b12
        m_im = a01 * b12 + b01 * a12
        q = h00 * h11 * h22 + 2.0 * (m_re * a02 + m_im * b02) - h00 * n12 - h11 * n02 - h22 * n01
        pq = p * q
        pp = p * p
        c0 = (1.0 - q * q * (1.0 / 720.0), pq * (1.0 / 120.0) - q * (1.0 / 6.0))
        c1 = (q * (1.0 / 24.0) - pq * (1.0 / 360.0), 1.0 - p * (1.0 / 6.0) + pp * (1.0 / 120.0))
        c2 = (p * (1.0 / 24.0) - 0.5 - pp * (1.0 / 720.0), q * (1.0 / 120.0))

        def cm(u, v):
            return (u[0] * v[0] - u[1] * v[1], u[0] * v[1] + u[1] * v[0])

        for _ in range(2):
            s00, s11, s22 = cm(c0, c0), cm(c1, c1), cm(c2, c2)
            d01, d02, d12 = cm(c0, c1), cm(c0, c2), cm(c1, c2)
            c0, c1, c2 = (
                tuple(s00[x] + 2.0 * q * d12[x] for x in range(2)),
                tuple(2.0 * (d01[x] + p * d12[x]) + q * s22[x] for x in range(2)),
                tuple(2.0 * d02[x] + s11[x] + p * s22[x] for x in range(2)),
            )
        g00 = h00 * h00 + n01 + n02
        g11 = h11 * h11 + n01 + n12
        g01 = (a01 * (h00 + h11) + a02 * a12 + b02 * b12, b01 * (h00 + h11) + b02 * a12 - a02 * b12)
        g02 = (a02 * (h00 + h22) + m_re, b02 * (h00 + h22) + m_im)
        g12 = (a12 * (h11 + h22) + a01 * a02 + b01 * b02, b12 * (h11 + h22) + a01 * b02 - b01 * a02)

        def mix(h, g):
            first, second = cm(c1, h), cm(c2, g)
            return (first[0] + second[0], first[1] + second[1])

        def diagonal(h, g):
            return (c0[0] + c1[0] * h + c2[0] * g, c0[1] + c1[1] * h + c2[1] * g)

        rotation = [
            [diagonal(h00, g00), mix((a01, b01), g01), mix((a02, b02), g02)],
            [mix((a01, -b01), (g01[0], -g01[1])), diagonal(h11, g11), mix((a12, b12), g12)],
        ]
        link = matrix_of(lambda e: links_ref[0, e, :, here])
        for r in range(2):
            for k in range(3):
                re, im = cdot(rotation[r], [link[m][k] for m in range(3)])
                new_ref[3 * r + k, :, here] = re
                new_ref[6 + 3 * r + k, :, here] = im
        return carry

    lax.fori_loop(0, tiles, one, 0)


def step_kernel(
    inner, outer, y_table,
    links_hbm, momentum_hbm, plane_hbm, modes_hbm, x_hbm, y_squares,
    new_ref, smooth_ref,
    links_ref, ahead_ref, momentum_ref, plane_ref, modes_ref, x_ref,
    high_ref, low_ref, weight_ref, path_ref, partial_ref, staple_ref, behind_ref,
    turn_x, turn_t, parts_out, parts_in, top_out, top_in, edge_out, edge_in,
    plane_sum_ref, spectrum_ref, both_ref, bands_ref, whole_ref, done_ref, back_ref, halves_ref, filtered_ref,
    load_sems, halo_sems, swap_sems, all_sems, ring_sems,
):
    me = lax.axis_index("gx")
    core = lax.axis_index("gy")
    other = 1 - core
    peers = inner * outer
    row = me // inner
    col = me % inner
    mesh_id = pl.DeviceIdType.MESH
    part = lax.axis_index("cfg")

    def wrapped(value, count):
        return lax.select(value >= count, value - count, value)

    def at(place):
        return (part, place, core)

    def in_row(step):
        return at(row * inner + wrapped(col + step % inner, inner))

    def in_column(step):
        return at(wrapped(row + step % outer, outer) * inner + col)

    before = at(wrapped(me + peers - 1, peers))
    after = at(wrapped(me + 1, peers))
    partner = (part, me, other)
    col_before, col_after = in_row(-1), in_row(1)
    row_before, row_after = in_column(-1), in_column(1)
    neighbours = (before, after, partner, col_before, col_after, row_before, row_after)

    def signal(sem, device):
        pl.semaphore_signal(sem, inc=1, device_id=device, device_id_type=mesh_id)

    def send(source, target, sems, device):
        return pltpu.make_async_remote_copy(
            src_ref=source, dst_ref=target, send_sem=sems.at[0], recv_sem=sems.at[1],
            device_id=device, device_id_type=mesh_id,
        )

    barrier = pltpu.get_barrier_semaphore()
    for device in neighbours:
        signal(barrier, device)
    loads = [
        pltpu.make_async_copy(links_hbm, links_ref, load_sems.at[0]),
        pltpu.make_async_copy(plane_hbm, plane_ref, load_sems.at[1]),
        pltpu.make_async_copy(modes_hbm.at[core], modes_ref, load_sems.at[2]),
        pltpu.make_async_copy(x_hbm, x_ref, load_sems.at[3]),
        pltpu.make_async_copy(momentum_hbm, momentum_ref, load_sems.at[4]),
    ]
    for load in loads:
        load.start()
    pl.semaphore_wait(barrier, len(neighbours))
    loads[0].wait()

    sites = new_ref.shape[2]
    halos = [send(links_ref.at[nu], ahead_ref.at[nu - 1], halo_sems.at[nu - 1], before) for nu in (1, 2)]
    quarters = 4
    width = sites // quarters
    quarter = [pl.ds(q * width, width) for q in range(quarters)]
    halos.append(send(links_ref.at[0], turn_x, halo_sems.at[2], after))
    for q in range(quarters):
        halos.append(
            send(links_ref.at[3, :, :, quarter[q]], turn_t.at[:, :, quarter[q]], halo_sems.at[3 + q], after)
        )
    for halo in halos:
        halo.start()

    def relay(count, known, place, stage):
        while known < count // 2:
            distance = max(known, 1)
            signal(ring_sems.at[stage], place(distance))
            signal(ring_sems.at[stage], place(-distance))
            pl.semaphore_wait(ring_sems.at[stage], 2)
            known += distance
            stage += 1
        return stage

    tiles = new_ref.shape[2] // LANES
    lane = lax.broadcasted_iota(jnp.int32, (8, LANES), 1)
    sublane = lax.broadcasted_iota(jnp.int32, (8, LANES), 0)
    t_site = lane % NT

    def lanes_of(i):
        return pl.ds(pl.multiple_of(i * LANES, LANES), LANES)


    def pack_top(i, carry):
        for e in range(12):
            top_out[e, pl.ds(i, 1), :] = links_ref[0, e, 0:1, lanes_of(i)]
        return carry

    lax.fori_loop(0, tiles, pack_top, 0)
    top = send(top_out, top_in, halo_sems.at[3 + quarters], partner)
    top.start()

    for load in loads[1:]:
        load.wait()

    def table_block(z, carry):
        full = plane_ref[0] * plane_ref[1, pl.ds(z, 1), :]
        high = full.astype(bf16)
        rows = pl.ds(pl.multiple_of(z * NT, NT), NT)
        high_ref[rows, :] = high
        low_ref[rows, :] = (full - high.astype(f32)).astype(bf16)
        return carry

    lax.fori_loop(0, NZ, table_block, 0)
    scale = 4.0 / (peers * inner * NZ * NT)
    weight_ref[...] = scale / (kernel_mass + 4.0 * (modes_ref[...] + y_squares[col]))
    last = relay(inner, 1, in_row, 0)
    top.wait()

    def prepare(i, carry):
        here = lanes_of(i)
        following = lanes_of(lax.rem(i + 1, tiles))

        def moved_y(e):
            edge = jnp.broadcast_to(top_in[e, pl.ds(i, 1), :], (8, LANES))
            return jnp.where(sublane == 7, edge, pltpu.roll(links_ref[0, e, :, here], 7, 0))

        def moved_z(e):
            return jnp.where(
                lane < LANES - NT,
                pltpu.roll(links_ref[0, e, :, here], LANES - NT, 1),
                pltpu.roll(links_ref[0, e, :, following], LANES - NT, 1),
            )

        for nu, moved in ((1, moved_y), (2, moved_z)):
            link_nu = matrix_of(lambda e: links_ref[nu, e, :, here])
            path = product(link_nu, matrix_of(moved))
            for r in range(3):
                for k in range(3):
                    path_ref[nu - 1, 3 * r + k, :, here] = path[r][k][0]
                    path_ref[nu - 1, 9 + 3 * r + k, :, here] = path[r][k][1]
        return carry

    lax.fori_loop(0, tiles, prepare, 0)

    def staples(nu, i):
        here = lanes_of(i)
        link_x = matrix_of(lambda e: links_ref[0, e, :, here])
        link_nu = matrix_of(lambda e: links_ref[nu, e, :, here])
        ahead = matrix_of(lambda e: ahead_ref[nu - 1, e, :, here])
        corner = product(link_x, ahead)
        lower = product(corner, link_nu, adj_left=True)
        path = [
            [(path_ref[nu - 1, 3 * r + k, :, here], path_ref[nu - 1, 9 + 3 * r + k, :, here]) for k in range(3)]
            for r in range(3)
        ]
        parts = algebra_parts(product(corner, path, adj_right=True))
        for a in range(8):
            if nu == 1:
                partial_ref[a, :, here] = parts[a]
            else:
                partial_ref[a, :, here] += parts[a]
        return here, [lower[r][k][p] for p in range(2) for r in range(3) for k in range(3)]

    def along_y(i, carry):
        here, flat = staples(1, i)
        for e in range(18):
            edge_out[e, pl.ds(i, 1), :] = flat[e][7:8, :]
            staple_ref[e, :, here] = jnp.where(sublane == 0, 0.0, pltpu.roll(flat[e], 1, 0))
        return carry

    def along_z(i, carry):
        here, flat = staples(2, i)
        for e in range(18):
            behind_ref[e, :, here] = flat[e]
        return carry

    def shift_t(value, forward):
        if forward:
            return jnp.where(
                t_site == NT - 1, pltpu.roll(value, NT - 1, 1), pltpu.roll(value, LANES - 1, 1)
            )
        return jnp.where(t_site == 0, pltpu.roll(value, LANES - NT + 1, 1), pltpu.roll(value, 1, 1))

    def along_t(i, carry):
        here = lanes_of(i)
        link_x = matrix_of(lambda e: turn_x[e, :, here])
        moved = matrix_of(lambda e: shift_t(turn_x[e, :, here], True))
        link_t = matrix_of(lambda e: turn_t[e, :, here])
        ahead = matrix_of(lambda e: links_ref[3, e, :, here])
        corner = product(link_x, ahead)
        lower = product(corner, link_t, adj_left=True)
        lower = [[tuple(shift_t(v, False) for v in entry) for entry in line] for line in lower]
        upper = algebra_parts(product(corner, product(link_t, moved), adj_right=True))
        below = algebra_parts(product(link_x, lower))
        for a in range(8):
            parts_out[a, :, here] = upper[a] + below[a]
        return carry

    halos[0].wait_recv()
    lax.fori_loop(0, tiles, along_y, 0)
    edge = send(edge_out, edge_in, halo_sems.at[4 + quarters], partner)
    edge.start()
    relay(outer, 0, in_column, last)
    per = tiles // quarters
    returned = []
    halos[2].wait_recv()
    for q in range(quarters):
        halos[3 + q].wait_recv()
        lax.fori_loop(per * q, per * (q + 1), along_t, 0)
        back = send(
            parts_out.at[:, :, quarter[q]], parts_in.at[:, :, quarter[q]],
            halo_sems.at[5 + quarters + q], before,
        )
        back.start()
        returned.append(back)
    halos[1].wait_recv()
    lax.fori_loop(0, tiles, along_z, 0)
    edge.wait()

    def force(i, carry):
        here = lanes_of(i)
        previous = lanes_of(lax.rem(i + tiles - 1, tiles))
        flat = [
            staple_ref[e, :, here]
            + jnp.where(sublane == 0, jnp.broadcast_to(edge_in[e, pl.ds(i, 1), :], (8, LANES)), 0.0)
            + jnp.where(
                lane >= NT,
                pltpu.roll(behind_ref[e, :, here], NT, 1),
                pltpu.roll(behind_ref[e, :, previous], NT, 1),
            )
            for e in range(18)
        ]
        staple = [[(flat[3 * r + k], flat[9 + 3 * r + k]) for k in range(3)] for r in range(3)]
        link_x = matrix_of(lambda e: links_ref[0, e, :, here])
        parts = algebra_parts(product(link_x, staple))
        for a in range(8):
            total = (coupling / 6.0) * (partial_ref[a, :, here] + parts[a] + parts_in[a, :, here])
            new_ref[a, :, here] = momentum_ref[a, :, here] - step_force * total
        return carry

    count = new_ref.shape[0] * new_ref.shape[1]
    half = tiles // 2
    for q in range(quarters):
        returned[q].wait_recv()
        lax.fori_loop(per * q, per * (q + 1), force, 0)
        taken = slice(q * width, (q + 1) * width)
        value = new_ref[:, :, taken].reshape(count, width)
        for pair in range(half):
            columns = slice(pair * 2 * LANES, (pair + 1) * 2 * LANES)
            out = split_dot(value, high_ref, low_ref, columns, taken)
            if q:
                out = out + plane_sum_ref[:, columns]
            if q < quarters - 1:
                plane_sum_ref[:, columns] = out
                continue
            for side in range(2):
                tile = 2 * pair + side
                spectrum_ref[tile // half, pl.ds(tile % half, count, stride=half), :] = out[
                    :, side * LANES : (side + 1) * LANES
                ]

    def swap(source, target, stage):
        remote = send(source.at[other], target.at[core], swap_sems.at[stage], partner)
        remote.start()
        local = pltpu.make_async_copy(source.at[core], target.at[core], swap_sems.at[stage, 2])
        local.start()
        local.wait()
        remote.wait()

    def all_to_all(source, target, stage):
        def push(to):
            send(source.at[to], target.at[me], all_sems.at[stage], at(to)).start()

        def begin(d, carry):
            push(wrapped(me + d, peers))
            push(wrapped(me + peers - d, peers))
            return carry

        lax.fori_loop(1, peers // 2, begin, 0)
        push(wrapped(me + peers // 2, peers))
        local = pltpu.make_async_copy(source.at[me], target.at[me], all_sems.at[stage, 2])
        local.start()
        local.wait()
        rest = pl.ds(0, peers - 1)
        pltpu.make_async_copy(source.at[rest], source.at[rest], all_sems.at[stage, 0]).wait()
        pltpu.make_async_copy(target.at[rest], target.at[rest], all_sems.at[stage, 1]).wait()

    swap(spectrum_ref, both_ref, 0)
    local_y = new_ref.shape[1]
    total_y = 2 * local_y

    def lines_of(c, y):
        return pl.ds(pl.multiple_of(c * (local_y * half), local_y * half) + (y % local_y) * half, half)

    def forward_y(c, carry):
        lines = [both_ref[y // local_y, lines_of(c, y), :] for y in range(total_y)]
        for k in range(total_y):
            total = None
            for y in range(total_y):
                term = float(y_table[k, y]) * lines[y]
                total = term if total is None else total + term
            bands_ref[c * inner + k] = total
        return carry

    lax.fori_loop(0, outer, forward_y, 0)
    all_to_all(bands_ref, whole_ref, 0)

    shape = whole_ref.shape
    flat_shape = (shape[0] * shape[1], shape[2])

    def transform(value):
        high = value.astype(bf16)
        low = (value - high.astype(f32)).astype(bf16)
        both = jnp.dot(x_ref[0], jnp.concatenate([high, low], axis=1), preferred_element_type=f32)
        rest = jnp.dot(x_ref[1], high, preferred_element_type=f32)
        return both[:, :LANES] + both[:, LANES:] + rest

    modes = transform(whole_ref[...].reshape(flat_shape)) * weight_ref[...]
    done_ref[...] = transform(modes).reshape(shape)
    all_to_all(done_ref, back_ref, 1)

    def inverse_y(c, carry):
        lines = [back_ref[c * inner + k] for k in range(total_y)]
        for y in range(total_y):
            total = None
            for k in range(total_y):
                term = float(y_table[k, y]) * lines[k]
                total = term if total is None else total + term
            halves_ref[y // local_y, lines_of(c, y), :] = total
        return carry

    lax.fori_loop(0, outer, inverse_y, 0)
    swap(halves_ref, filtered_ref, 1)
    value = jnp.concatenate(
        [filtered_ref[tile // half, pl.ds(tile % half, count, stride=half), :] for tile in range(tiles)],
        axis=1,
    )
    for pair in range(half):
        columns = slice(pair * 2 * LANES, (pair + 1) * 2 * LANES)
        smooth_ref[:, columns] = split_dot(value, high_ref, low_ref, columns)
    for halo in halos + returned:
        halo.wait_send()


def sine_squares(length):
    return np.sin(np.pi * np.arange(length) / length) ** 2


def shards(gauge_links, momentum):
    channels, _, local_y, sites = momentum.shape
    gx_count = lax.axis_size("gx")
    inner = 2 * local_y
    outer = channels
    tiles = sites // LANES
    half = tiles // 2
    rows = channels * local_y
    links = gauge_links.reshape(4, 12, local_y, sites)
    field = (channels, local_y, sites)

    plane = np.stack([np.tile(hartley(NT), (1, NZ)), np.repeat(hartley(NZ), NT, axis=1)]).astype(np.float32)
    index = np.arange(sites)
    z_t = (sine_squares(NZ)[index // NT] + sine_squares(NT)[index % NT]).reshape(2, half, LANES)
    modes = np.tile(z_t, (1, gx_count, 1)) + np.repeat(sine_squares(gx_count), half)[None, :, None]
    x_high, x_low = in_two(np.kron(hartley(gx_count), np.eye(half)).astype(np.float32))
    x_table = jnp.stack([x_high, x_low])
    y_squares = jnp.asarray(sine_squares(inner), f32)

    any_spec = pl.BlockSpec(memory_space=pl.ANY)
    exchanged = (gx_count, half, LANES)
    halved = (2, rows * half, LANES)
    staple = (18, local_y, sites)
    new_momentum, smooth = pl.pallas_call(
        functools.partial(step_kernel, inner, outer, hartley(inner)),
        out_shape=[jax.ShapeDtypeStruct(field, f32), jax.ShapeDtypeStruct((rows, sites), f32)],
        in_specs=[any_spec] * 5 + [pl.BlockSpec(memory_space=pltpu.SMEM)],
        out_specs=[VMEM] * 2,
        scratch_shapes=[
            pltpu.VMEM(links.shape, f32),
            pltpu.VMEM((2,) + links.shape[1:], f32),
            pltpu.VMEM(field, f32),
            pltpu.VMEM(plane.shape, f32),
            pltpu.VMEM(modes.shape[1:], f32),
            pltpu.VMEM(x_table.shape, bf16),
            pltpu.VMEM((sites, sites), bf16),
            pltpu.VMEM((sites, sites), bf16),
            pltpu.VMEM(modes.shape[1:], f32),
            pltpu.VMEM((2,) + staple, f32),
            pltpu.VMEM(field, f32),
            pltpu.VMEM(staple, f32),
            pltpu.VMEM(staple, f32),
            pltpu.VMEM(links.shape[1:], f32),
            pltpu.VMEM(links.shape[1:], f32),
            pltpu.VMEM(field, f32),
            pltpu.VMEM(field, f32),
            pltpu.VMEM((12, tiles, LANES), f32),
            pltpu.VMEM((12, tiles, LANES), f32),
            pltpu.VMEM((18, tiles, LANES), f32),
            pltpu.VMEM((18, tiles, LANES), f32),
            pltpu.VMEM((rows, sites), f32),
            pltpu.VMEM(halved, f32),
            pltpu.VMEM(halved, f32),
            pltpu.VMEM(exchanged, f32),
            pltpu.VMEM(exchanged, f32),
            pltpu.VMEM(exchanged, f32),
            pltpu.VMEM(exchanged, f32),
            pltpu.VMEM(halved, f32),
            pltpu.VMEM(halved, f32),
            pltpu.SemaphoreType.DMA((5,)),
            pltpu.SemaphoreType.DMA((13, 2)),
            pltpu.SemaphoreType.DMA((2, 3)),
            pltpu.SemaphoreType.DMA((2, 3)),
            pltpu.SemaphoreType.REGULAR((2 * gx_count.bit_length(),)),
        ],
        compiler_params=pltpu.CompilerParams(collective_id=0, has_side_effects=True, **PARAMS),
        name="momentum_and_smooth",
    )(links, momentum.reshape(field), jnp.asarray(plane), jnp.asarray(modes, f32), x_table, y_squares)

    width = 2 * LANES
    new_link, new_momentum = pl.pallas_call(
        finish_kernel,
        grid=(sites // width,),
        out_shape=[jax.ShapeDtypeStruct(links.shape[1:], f32), jax.ShapeDtypeStruct(field, f32)],
        in_specs=[
            pl.BlockSpec((rows, width), lambda i: (0, i)),
            pl.BlockSpec((1, 12, local_y, width), lambda i: (0, 0, 0, i)),
            pl.BlockSpec((channels, local_y, width), lambda i: (0, 0, i)),
        ],
        out_specs=[
            pl.BlockSpec((12, local_y, width), lambda i: (0, 0, i)),
            pl.BlockSpec((channels, local_y, width), lambda i: (0, 0, i)),
        ],
        compiler_params=pltpu.CompilerParams(**PARAMS),
        name="link_update",
    )(smooth, links, new_momentum)
    return (new_momentum.reshape(momentum.shape), new_link.reshape(12, 1, local_y, sites))


def solution(mesh):
    return jax.shard_map(
        shards,
        mesh=mesh,
        in_specs=(P(None, None, ("cfg", "gx"), "gy", None), P(None, ("cfg", "gx"), "gy", None)),
        out_specs=(P(None, ("cfg", "gx"), "gy", None), P(None, ("cfg", "gx"), "gy", None)),
        check_vma=False,
    )
```
